512 devices in a mesh: groups: 2 (over y), src: 64 (over z, core), act: 4 (over x).
Axes of the slice: x: 4, y: 2, z: 32, core: 2. Of those that a mesh axis runs over, the one named last changes fastest.
The devices are a block of a 4x8x32 slice.
Arguments:
- star_state: float32 [12, 65536], P(None, ('groups', 'src')), parts along dimension 1, may hold values from -6 to 6
- masses: float32 [65536], P(('groups', 'src')), parts along dimension 0, may hold values from 0.25 to 4
- phases: float32 [65536], P(('groups', 'src')), parts along dimension 0, may hold values from 0 to 1
- levels: int32 [65536], P(('groups', 'src')), parts along dimension 0, may hold values from 0 to 4, as said below
- active_list: int32 [32768], P(('groups', 'src', 'act')), parts along dimension 0, may hold values from 0 to 511, as said below
- active_count: int32 [512], P(('groups', 'src', 'act')), parts along dimension 0, may hold values from 0 to 64, as said below
Outputs:
- stepped_state: float32 [12, 65536], P(None, ('groups', 'src')), parts along dimension 1
The draws below stay inside these ranges and needn't reach their ends.
There are 2 independent parts, one for each index of `groups`. The reference program is written for one: setup_inputs(seed, part) draws one part's arguments, and reference() takes and returns one part's arrays. A program takes and returns all parts, laid end to end along the dimension named above; each array names one. Nothing has to cross between parts.
Inputs may be any that keep to these rules, and one draw needn't show every extreme that they name: `levels`: levels_j = 4 exactly for the stars that appear among the live entries of the lists. `active_list`: live entries (the first active_count ones of a device's 64) are distinct indices within the device's src shard; every active star of a shard is live in exactly one list of that shard's 4 devices; later slots hold arbitrary indices of the shard. `active_count`: at most 64 a device, reached in every draw; the counts of one src shard's devices sum to at most 128, reached by some shard in every draw.
All inputs are finite; a program needn't handle non-finite values.
Results may differ from the reference program's by a relative error of at most 0.0003.
Values sent between devices are 32-bit elements; how exact they have to be, the bound alone decides.
A program may use at most 64 MiB of HBM per device.

```python
import math
import jax
import jax.numpy as jnp
from jax import lax

S_DEV = 512
A_SLOT = 64
LEVELS = 5
STEPS = 2
NSTARS = 32768
N_SRC = 64
N_ACT = 4


def layout(key):
    shards = NSTARS // S_DEV
    base = jax.random.fold_in(key, 7)
    keys = jax.random.split(base, 8)
    cap = A_SLOT
    first = jax.random.randint(keys[0], (shards,), cap // 4, cap + 1, dtype=jnp.int32)
    second = jax.random.randint(keys[1], (shards,), 0, cap + 1, dtype=jnp.int32)
    third = jax.random.randint(keys[2], (shards,), 0, jnp.minimum(cap, 2 * cap - first - second) + 1, dtype=jnp.int32)
    fourth = jax.random.randint(keys[3], (shards,), 0, jnp.minimum(cap, 2 * cap - first - second - third) + 1, dtype=jnp.int32)
    full_shard = jax.random.randint(keys[4], (), 0, shards, dtype=jnp.int32)
    is_full = jnp.arange(shards, dtype=jnp.int32) == full_shard
    first = jnp.where(is_full, cap, first)
    second = jnp.where(is_full, cap, second)
    third = jnp.where(is_full, 0, third)
    fourth = jnp.where(is_full, 0, fourth)
    grouped = jnp.stack([first, second, third, fourth], axis=1)
    scores = jax.random.randint(keys[5], (shards, 4), 0, 65536, dtype=jnp.int32) * 4 + jnp.arange(4, dtype=jnp.int32)[None, :]
    order = jnp.argsort(scores, axis=1)
    counts = jnp.take_along_axis(grouped, order, axis=1).astype(jnp.int32)
    totals = jnp.sum(counts, axis=1)
    star_scores = jax.random.randint(keys[6], (shards, S_DEV), 0, 65536, dtype=jnp.int32) * S_DEV + jnp.arange(S_DEV, dtype=jnp.int32)[None, :]
    chosen = jnp.argsort(star_scores, axis=1).astype(jnp.int32)
    rank_of = jnp.argsort(chosen, axis=1).astype(jnp.int32)
    list_starts = jnp.cumsum(counts, axis=1) - counts
    position = (list_starts[:, :, None] + jnp.arange(cap, dtype=jnp.int32)[None, None, :]) % S_DEV
    lists = jnp.take_along_axis(chosen, position.reshape(shards, 4 * cap), axis=1).astype(jnp.int32)
    coarse = jax.random.randint(keys[7], (shards, S_DEV), 0, LEVELS - 1, dtype=jnp.int32)
    level_table = jnp.where(rank_of < totals[:, None], LEVELS - 1, coarse).astype(jnp.int32)
    return (level_table.reshape(-1), lists.reshape(-1), counts.reshape(-1))


def draw_levels(key, part):
    return layout(key)[0]


def draw_active_list(key, part):
    return layout(key)[1]


def draw_active_count(key, part):
    return layout(key)[2]


def block_scale(key, extent, cuts, least, high):
    gain = 1.0
    for dim, shards_of in cuts:
        steps = jax.random.uniform(jax.random.fold_in(jax.random.fold_in(key, 6), dim), (shards_of,), jnp.float32, least / len(cuts), high / len(cuts))
        gain = gain * jnp.repeat(jnp.exp(steps), extent[dim] // shards_of).reshape((-1,) + (1,) * (len(extent) - 1 - dim))
    return gain


def centred(stream_key, dims, spread, reach, cuts=(), kind=jnp.bfloat16):
    entries = jax.random.normal(stream_key, dims, jnp.float32) * spread
    if len(cuts) > 0:
        entries = block_scale(stream_key, dims, cuts, -0.22, 0.18) * entries
    return jnp.clip(entries, min=-reach, max=reach).astype(kind)


def setup_inputs(seed: int = 0, part: int = 0) -> dict:
    streams_of = jax.random.split(jax.random.key(seed), 7)
    part_keys = jax.random.split(jax.random.fold_in(streams_of[6], part), 7)
    star_state = centred(part_keys[0], (12, NSTARS), 1.0, 6.0, ((1, 64),), jnp.float32)
    masses = jnp.clip(jnp.exp(math.log(4.0) - 2.7725887 * jax.random.uniform(part_keys[1], (NSTARS,), jnp.float32) ** block_scale(part_keys[1], (NSTARS,), ((0, 64),), -0.2, 0.2)), 0.25, 4.0)
    phases = jnp.clip(1.0 * jax.random.uniform(part_keys[2], (NSTARS,), jnp.float32) ** block_scale(part_keys[2], (NSTARS,), ((0, 64),), -0.2, 0.2), 0.0, 1.0)
    levels = draw_levels(jax.random.fold_in(jax.random.fold_in(streams_of[6], part), 71), part)
    active_list = draw_active_list(jax.random.fold_in(jax.random.fold_in(streams_of[6], part), 71), part)
    active_count = draw_active_count(jax.random.fold_in(jax.random.fold_in(streams_of[6], part), 71), part)
    return {"star_state": star_state, "masses": masses, "phases": phases, "levels": levels, "active_list": active_list, "active_count": active_count}


soften_sq = 0.0004
fine_step = 0.03125

def predict(star_state, elapsed):
    interval = elapsed[None, :]
    position = star_state[0:3] + interval * (star_state[3:6] + interval * (0.5 * star_state[6:9] + interval * star_state[9:12] / 6.0))
    velocity = star_state[3:6] + interval * (star_state[6:9] + 0.5 * interval * star_state[9:12])
    return jnp.concatenate([position, velocity], axis=0)

def pair_block(targets, sources):
    delta_pos = sources[0:3, None, :] - targets[0:3, :, None]
    delta_vel = sources[3:6, None, :] - targets[3:6, :, None]
    dist_sq = delta_pos[0] * delta_pos[0] + delta_pos[1] * delta_pos[1] + delta_pos[2] * delta_pos[2] + soften_sq
    inverse = lax.rsqrt(dist_sq)
    inv_sq = inverse * inverse
    weight = sources[6][None, :] * inverse * inv_sq
    radial = (delta_pos[0] * delta_vel[0] + delta_pos[1] * delta_vel[1] + delta_pos[2] * delta_vel[2]) * inv_sq * 3.0
    acceleration = lax.optimization_barrier(jnp.sum(weight[None] * delta_pos, axis=2))
    jerk_sum = lax.optimization_barrier(jnp.sum(weight[None] * (delta_vel - radial[None] * delta_pos), axis=2))
    return jnp.concatenate([acceleration, jerk_sum], axis=0)

def over_sources(targets, sources):
    count_src = sources.shape[1]
    width = 512
    if count_src > width and count_src % width == 0:
        blocks = sources.reshape(7, count_src // width, width).transpose(1, 0, 2)

        def accumulate(running, portion):
            return (running + pair_block(targets, portion), None)
        init = jnp.zeros((6, targets.shape[1]), jnp.float32)
        running, unused = lax.scan(accumulate, init, blocks)
        return running
    return pair_block(targets, sources)

def pair_forces(targets, sources):
    count_tgt = targets.shape[1]
    width = 512
    if count_tgt > width and count_tgt % width == 0:
        blocks = targets.reshape(6, count_tgt // width, width).transpose(1, 0, 2)
        result = lax.map(lambda portion: over_sources(portion, sources), blocks)
        return result.transpose(1, 0, 2).reshape(6, count_tgt)
    return over_sources(targets, sources)

def correct(old_state, predicted_rows, forces):
    step_len = fine_step
    acc_old = old_state[6:9]
    jerk_old = old_state[9:12]
    acc_new = forces[0:3]
    jerk_new = forces[3:6]
    snap_term = (-6.0 * (acc_old - acc_new) - step_len * (4.0 * jerk_old + 2.0 * jerk_new)) / (step_len * step_len)
    crackle = (12.0 * (acc_old - acc_new) + 6.0 * step_len * (jerk_old + jerk_new)) / (step_len * step_len * step_len)
    position = predicted_rows[0:3] + step_len ** 4 / 24.0 * snap_term + step_len ** 5 / 120.0 * crackle
    velocity = predicted_rows[3:6] + step_len ** 3 / 6.0 * snap_term + step_len ** 4 / 24.0 * crackle
    return jnp.concatenate([position, velocity, acc_new, jerk_new], axis=0)

def reference(star_state, masses, phases, levels, active_list, active_count):
    lists = active_list.reshape(N_SRC, N_ACT, A_SLOT).astype(jnp.int32)
    counts = active_count.reshape(N_SRC, N_ACT).astype(jnp.int32)
    list_ends = jnp.cumsum(counts, axis=1)
    list_starts = list_ends - counts
    totals = list_ends[:, -1]
    slot_index = jnp.arange(A_SLOT, dtype=jnp.int32)
    position = jnp.where(slot_index[None, None, :] < counts[:, :, None], list_starts[:, :, None] + slot_index[None, None, :], 2 * A_SLOT)
    shard_index = jnp.broadcast_to(jnp.arange(N_SRC, dtype=jnp.int32)[:, None, None], position.shape)
    compact = jnp.zeros((N_SRC, 2 * A_SLOT + 1), jnp.int32).at[shard_index, position].set(lists)[:, :2 * A_SLOT]
    live = jnp.arange(2 * A_SLOT, dtype=jnp.int32)[None, :] < totals[:, None]
    members = (jnp.arange(N_SRC, dtype=jnp.int32)[:, None] * S_DEV + compact).reshape(-1)
    write_index = jnp.where(live.reshape(-1), members, NSTARS).astype(jnp.int32)
    weights = masses / NSTARS
    tick_count = jnp.left_shift(jnp.int32(1), (LEVELS - 1 - levels).astype(jnp.int32)).astype(jnp.float32)
    state_now = star_state
    for substep in range(STEPS):
        elapsed = jnp.where(levels == LEVELS - 1, 1.0, phases * (tick_count - STEPS) + (substep + 1)) * fine_step
        predicted = predict(state_now, elapsed)
        sources = jnp.concatenate([predicted, weights[None, :]], axis=0)
        targets = predicted[:, members]
        forces = pair_forces(targets, sources)
        new_state = correct(state_now[:, members], targets, forces)
        state_now = state_now.at[:, write_index].set(new_state, mode='drop')
    return state_now
```

```python
import functools

import jax
import jax.numpy as jnp
from jax import lax
from jax.experimental import pallas as pl
from jax.experimental.pallas import tpu as pltpu
from jax.sharding import PartitionSpec as P

LEVELS = 5
STEPS = 2
SPAN = 8

soften_sq = 0.0004
fine_step = 0.03125
MESH = pl.DeviceIdType.MESH
HIGHEST = lax.Precision.HIGHEST


def predict(pos, vel, acc, jerk, interval):
    new_pos = pos + interval * (vel + interval * (0.5 * acc + interval * jerk / 6.0))
    new_vel = vel + interval * (acc + 0.5 * interval * jerk)
    return new_pos, new_vel


def correct(acc_old, jerk_old, acc_new, jerk_new, pos_pred, vel_pred):
    snap_term = (-6.0 * (acc_old - acc_new) - fine_step * (4.0 * jerk_old + 2.0 * jerk_new)) / (
        fine_step * fine_step
    )
    crackle = (12.0 * (acc_old - acc_new) + 6.0 * fine_step * (jerk_old + jerk_new)) / (
        fine_step * fine_step * fine_step
    )
    pos = pos_pred + fine_step**4 / 24.0 * snap_term + fine_step**5 / 120.0 * crackle
    vel = vel_pred + fine_step**3 / 6.0 * snap_term + fine_step**4 / 24.0 * crackle
    return pos, vel


def spread(tile, wide):
    stars = tile.shape[1]
    columns = jnp.transpose(tile)
    for row in range(7):
        wide[row, 0:stars, :] = jnp.broadcast_to(columns[:, row : row + 1], (stars, 128))


def accumulate(wide, begin, count, targets, sums, pair, first):
    aim = [
        [jnp.broadcast_to(targets[2 * pair + i, row : row + 1, :], (8, 128)) for row in range(6)]
        for i in range(2)
    ]

    def body(step, totals):
        rows = pl.ds(pl.multiple_of(begin + step * 8, 8), 8)
        source = [wide[row, rows, :] for row in range(7)]
        finished = []
        for i in range(2):
            dx, dy, dz, du, dv, dw = [source[row] - aim[i][row] for row in range(6)]
            dist_sq = dx * dx + dy * dy + dz * dz + soften_sq
            inverse = lax.rsqrt(dist_sq)
            inv_sq = inverse * inverse
            weight = source[6] * inverse * inv_sq
            radial = (dx * du + dy * dv + dz * dw) * inv_sq * 3.0
            part = [weight * d for d in (dx, dy, dz)]
            part += [weight * (e - radial * d) for d, e in ((dx, du), (dy, dv), (dz, dw))]
            finished += part
        return tuple(t + p for t, p in zip(totals, finished))

    if first:
        totals = tuple(jnp.zeros((8, 128), jnp.float32) for _ in range(12))
    else:
        totals = tuple(sums[2 * pair + i, row] for i in range(2) for row in range(6))
    totals = lax.fori_loop(0, count // 8, body, totals, unroll=2)
    for i in range(2):
        for row in range(6):
            sums[2 * pair + i, row] = totals[6 * i + row]


def kernel(
    n_src,
    n_act,
    state_ref,
    mass_ref,
    phase_ref,
    level_ref,
    out_ref,
    own0,
    own1,
    tile_a,
    tile_b,
    got0,
    got1,
    got_act,
    aim0,
    aim1,
    wide,
    sums,
    give0,
    give1,
    take0,
    take1,
    line0,
    line1,
    lines0,
    lines1,
    hot,
    held,
    send_sem,
    recv_sem,
):
    n_col = n_src // SPAN
    me = lax.axis_index("src")
    act = lax.axis_index("act")
    place = lax.rem(me, SPAN)
    base = me - place
    stars = state_ref.shape[1]
    part = stars // n_act
    slots = hot.shape[0]

    col_peer = [{"src": lax.rem(me + SPAN * q, n_src), "act": act} for q in range(n_col)]
    row_peer = [{"src": base + lax.rem(place + r, SPAN), "act": act} for r in range(SPAN)]
    act_peer = [{"src": me, "act": lax.rem(act + i, n_act)} for i in range(n_act)]

    barrier = pltpu.get_barrier_semaphore()
    everyone = col_peer[1:] + row_peer[1:] + act_peer[1:]
    for peer in everyone:
        pl.semaphore_signal(barrier, inc=1, device_id=peer, device_id_type=MESH)

    counter = [0]

    def exchange(peers, source, target, rows=8):
        n = len(peers)
        copies = [None] * n
        for k in range(1, n):
            copies[n - k] = pltpu.make_async_remote_copy(
                src_ref=source(k),
                dst_ref=target.at[n - k, 0:rows],
                send_sem=send_sem.at[counter[0] + k],
                recv_sem=recv_sem.at[counter[0] + n - k],
                device_id=peers[k],
                device_id_type=MESH,
            )
        counter[0] += n
        return copies

    total = jnp.float32(stars * n_src)
    mine = pl.ds(pl.multiple_of(act * part, part), part)
    level = level_ref[:, mine]
    tick_count = jnp.left_shift(jnp.int32(1), LEVELS - 1 - level).astype(jnp.float32)
    weight = mass_ref[:, mine] / total
    for substep, own in ((0, own0), (1, own1)):
        elapsed = (
            jnp.where(
                level == LEVELS - 1,
                1.0,
                phase_ref[:, mine] * (tick_count - STEPS) + (substep + 1),
            )
            * fine_step
        )
        pos, vel = predict(
            state_ref[0:3, mine],
            state_ref[3:6, mine],
            state_ref[6:9, mine],
            state_ref[9:12, mine],
            elapsed,
        )
        own[0:3, :] = pos
        own[3:6, :] = vel
        own[6:7, :] = weight if substep == 0 else jnp.where(level == LEVELS - 1, 0.0, weight)
        own[7:8, :] = jnp.zeros((1, part), jnp.float32)

    is_active = level_ref[...] == LEVELS - 1
    flags = jnp.broadcast_to(jnp.where(is_active, 1.0, 0.0), (8, stars))
    before = lax.broadcasted_iota(jnp.int32, (stars, stars), 0) < lax.broadcasted_iota(
        jnp.int32, (stars, stars), 1
    )
    rank = jnp.dot(
        flags.astype(jnp.bfloat16),
        jnp.where(before, 1.0, 0.0).astype(jnp.bfloat16),
        preferred_element_type=jnp.float32,
    )[0:1, :]
    rank = jnp.where(is_active, rank, float(slots)).astype(jnp.int32)
    hot[...] = jnp.where(
        lax.broadcasted_iota(jnp.int32, (slots, stars), 0) == rank, 1.0, 0.0
    )
    over_stars = (((1,), (1,)), ((), ()))
    held[0:12, :] = lax.dot_general(
        state_ref[...], hot[...], over_stars, precision=HIGHEST, preferred_element_type=jnp.float32
    )
    held_mass = lax.dot_general(
        jnp.broadcast_to(mass_ref[...] / total, (8, stars)),
        hot[...],
        over_stars,
        precision=HIGHEST,
        preferred_element_type=jnp.float32,
    )[0:1, :]

    def predict_held(tile):
        pos, vel = predict(
            held[0:3, :], held[3:6, :], held[6:9, :], held[9:12, :], fine_step
        )
        tile[0:3, :] = pos
        tile[3:6, :] = vel
        tile[6:7, :] = held_mass
        tile[7:8, :] = jnp.zeros((1, slots), jnp.float32)

    predict_held(tile_a)
    aim0[0] = tile_a[...]
    spread(own0[...], wide)

    pl.semaphore_wait(barrier, len(everyone))
    cols0 = exchange(col_peer, lambda k: own0, got0)
    rows0 = exchange(row_peer, lambda k: tile_a, aim0)
    order = sorted(range(1, n_col), key=lambda q: -min(q, n_col - q))
    for q in order:
        cols0[q].start()
    for copy in rows0[1:]:
        copy.start()
    cols1 = exchange(col_peer, lambda k: own1, got1)

    def over_pairs(begin, count, targets, first):
        def one(pair, carry):
            accumulate(wide, begin, count, targets, sums, pair, first)
            return carry

        lax.fori_loop(0, SPAN // 2, one, 0)

    def last_block(begin, count, targets, give, copies):
        for pair in reversed(range(SPAN // 2)):
            accumulate(wide, begin, count, targets, sums, pair, False)
            for k in (2 * pair, 2 * pair + 1):
                for row in range(6):
                    give[k, row : row + 1, :] = jnp.sum(sums[k, row], axis=0, keepdims=True)
                if k > 0:
                    copies[SPAN - k].start()

    def reduced(give, take, copies, line, lines, act_copies):
        for copy in copies[1:]:
            copy.wait_recv()
        summed = give[0, 0:6, :]
        for r in range(1, SPAN):
            summed = summed + take[r, 0:6, :]
        line[0:6, :] = summed
        for copy in act_copies[1:]:
            copy.start()
        for copy in act_copies[1:]:
            copy.wait_recv()
        near = [summed] + [lines[i, 0:6, :] for i in range(1, n_act)]
        while len(near) > 1:
            half = len(near) // 2
            near = [near[i] + near[i + half] for i in range(half)]
        return near[0]

    def corrected(forces, tile):
        acc_old, jerk_old = held[6:9, :], held[9:12, :]
        acc_new, jerk_new = forces[0:3, :], forces[3:6, :]
        pos, vel = correct(acc_old, jerk_old, acc_new, jerk_new, tile[0:3, :], tile[3:6, :])
        held[0:3, :] = pos
        held[3:6, :] = vel
        held[6:9, :] = acc_new
        held[9:12, :] = jerk_new

    for copy in rows0[1:]:
        copy.wait_recv()
    over_pairs(0, part, aim0, True)
    arrival = order[::-1]
    gives0 = exchange(row_peer, lambda k: give0.at[k, 0:6], take0, 6)
    acts0 = exchange(act_peer, lambda k: line0.at[0:6], lines0, 6)
    for n, q in enumerate(arrival):
        cols0[q].wait_recv()
        spread(got0[q], wide)
        if q != arrival[-1]:
            over_pairs(0, part, aim0, False)
        else:
            last_block(0, part, aim0, give0, gives0)
        if n == 1:
            for copy in cols1[1:]:
                copy.start()
    corrected(reduced(give0, take0, gives0, line0, lines0, acts0), tile_a)

    predict_held(tile_b)
    cols2 = exchange(col_peer, lambda k: tile_b, got_act)
    rows1 = exchange(row_peer, lambda k: tile_b, aim1)
    for copy in rows1[1:]:
        copy.start()
    for q in order:
        cols2[q].start()
    aim1[0] = tile_b[...]
    spread(own1[...], wide)
    for copy in rows1[1:]:
        copy.wait_recv()
    over_pairs(0, part, aim1, True)
    for q in arrival:
        cols1[q].wait_recv()
        spread(got1[q], wide)
        over_pairs(0, part, aim1, False)
    share = slots // n_act
    first_slot = act * share
    spread(tile_b[...], wide)
    over_pairs(first_slot, share, aim1, False)
    gives1 = exchange(row_peer, lambda k: give1.at[k, 0:6], take1, 6)
    acts1 = exchange(act_peer, lambda k: line1.at[0:6], lines1, 6)
    for q in arrival:
        cols2[q].wait_recv()
        spread(got_act[q], wide)
        if q != arrival[-1]:
            over_pairs(first_slot, share, aim1, False)
        else:
            last_block(first_slot, share, aim1, give1, gives1)
    corrected(reduced(give1, take1, gives1, line1, lines1, acts1), tile_b)

    moved = jnp.dot(held[...], hot[...], precision=HIGHEST, preferred_element_type=jnp.float32)
    out_ref[...] = jnp.where(is_active, moved[0:12, :], state_ref[...])
    for copies in (cols0, rows0, cols1, gives0, acts0, cols2, rows1, gives1, acts1):
        for copy in copies[1:]:
            copy.wait_send()


def solution(mesh):
    n_src, n_act = mesh.shape["src"], mesh.shape["act"]
    n_col = n_src // SPAN

    def per_device(star_state, masses, phases, levels, active_list, active_count):
        stars = star_state.shape[1]
        part = stars // n_act
        slots = 2 * active_list.shape[0]
        vmem = pl.BlockSpec(memory_space=pltpu.VMEM)
        n_sem = 3 * n_col + 4 * SPAN + 2 * n_act

        def tiles(*lead):
            return pltpu.VMEM((*lead, 8, 128), jnp.float32)

        return pl.pallas_call(
            functools.partial(kernel, n_src, n_act),
            out_shape=jax.ShapeDtypeStruct(star_state.shape, jnp.float32),
            in_specs=[vmem] * 4,
            out_specs=vmem,
            scratch_shapes=[
                pltpu.VMEM((8, part), jnp.float32),
                pltpu.VMEM((8, part), jnp.float32),
                pltpu.VMEM((8, slots), jnp.float32),
                pltpu.VMEM((8, slots), jnp.float32),
                pltpu.VMEM((n_col, 8, part), jnp.float32),
                pltpu.VMEM((n_col, 8, part), jnp.float32),
                pltpu.VMEM((n_col, 8, slots), jnp.float32),
                pltpu.VMEM((SPAN, 8, slots), jnp.float32),
                pltpu.VMEM((SPAN, 8, slots), jnp.float32),
                pltpu.VMEM((8, max(part, slots), 128), jnp.float32),
                tiles(SPAN, 6),
                tiles(SPAN),
                tiles(SPAN),
                tiles(SPAN),
                tiles(SPAN),
                tiles(),
                tiles(),
                tiles(n_act),
                tiles(n_act),
                pltpu.VMEM((slots, stars), jnp.float32),
                pltpu.VMEM((12, slots), jnp.float32),
                pltpu.SemaphoreType.DMA((n_sem,)),
                pltpu.SemaphoreType.DMA((n_sem,)),
            ],
            compiler_params=pltpu.CompilerParams(collective_id=0, has_side_effects=True),
        )(
            star_state,
            masses.reshape(1, stars),
            phases.reshape(1, stars),
            levels.reshape(1, stars),
        )

    in_specs = (
        P(None, ("groups", "src")),
        P(("groups", "src")),
        P(("groups", "src")),
        P(("groups", "src")),
        P(("groups", "src", "act")),
        P(("groups", "src", "act")),
    )
    return jax.shard_map(
        per_device,
        mesh=mesh,
        in_specs=in_specs,
        out_specs=P(None, ("groups", "src")),
        check_vma=False,
    )
```

```python
import functools

import jax
import jax.numpy as jnp
from jax import lax
from jax.experimental import pallas as pl
from jax.experimental.pallas import tpu as pltpu
from jax.sharding import PartitionSpec as P

LEVELS = 5
STEPS = 2
SPAN = 8

soften_sq = 0.0004
fine_step = 0.03125
MESH = pl.DeviceIdType.MESH
HIGHEST = lax.Precision.HIGHEST


def predict(pos, vel, acc, jerk, interval):
    new_pos = pos + interval * (vel + interval * (0.5 * acc + interval * jerk / 6.0))
    new_vel = vel + interval * (acc + 0.5 * interval * jerk)
    return new_pos, new_vel


def correct(acc_old, jerk_old, acc_new, jerk_new, pos_pred, vel_pred):
    snap_term = (-6.0 * (acc_old - acc_new) - fine_step * (4.0 * jerk_old + 2.0 * jerk_new)) / (
        fine_step * fine_step
    )
    crackle = (12.0 * (acc_old - acc_new) + 6.0 * fine_step * (jerk_old + jerk_new)) / (
        fine_step * fine_step * fine_step
    )
    pos = pos_pred + fine_step**4 / 24.0 * snap_term + fine_step**5 / 120.0 * crackle
    vel = vel_pred + fine_step**3 / 6.0 * snap_term + fine_step**4 / 24.0 * crackle
    return pos, vel


def spread(tile, wide):
    stars = tile.shape[1]
    columns = jnp.transpose(tile)
    for row in range(7):
        wide[row, 0:stars, :] = jnp.broadcast_to(columns[:, row : row + 1], (stars, 128))


def spread_part(tile, columns, begin, count, wide, at):
    columns[...] = jnp.transpose(tile)
    chosen = columns[pl.ds(pl.multiple_of(begin, count), count), :]
    for row in range(7):
        wide[row, at : at + count, :] = jnp.broadcast_to(chosen[:, row : row + 1], (count, 128))


def accumulate(wide, count, targets, sums, pair, first):
    aim = [
        [jnp.broadcast_to(targets[2 * pair + i, row : row + 1, :], (8, 128)) for row in range(6)]
        for i in range(2)
    ]

    def body(step, totals):
        rows = pl.ds(pl.multiple_of(step * 8, 8), 8)
        source = [wide[row, rows, :] for row in range(7)]
        finished = []
        for i in range(2):
            dx, dy, dz, du, dv, dw = [source[row] - aim[i][row] for row in range(6)]
            dist_sq = dx * dx + dy * dy + dz * dz + soften_sq
            inverse = lax.rsqrt(dist_sq)
            inv_sq = inverse * inverse
            weight = source[6] * inverse * inv_sq
            radial = (dx * du + dy * dv + dz * dw) * inv_sq * 3.0
            part = [weight * d for d in (dx, dy, dz)]
            part += [weight * (e - radial * d) for d, e in ((dx, du), (dy, dv), (dz, dw))]
            finished += part
        return tuple(t + p for t, p in zip(totals, finished))

    if first:
        totals = tuple(jnp.zeros((8, 128), jnp.float32) for _ in range(12))
    else:
        totals = tuple(sums[2 * pair + i, row] for i in range(2) for row in range(6))
    totals = lax.fori_loop(0, count // 8, body, totals, unroll=2)
    for i in range(2):
        for row in range(6):
            sums[2 * pair + i, row] = totals[6 * i + row]


def flipped(place, r):
    result, bit = place, 1
    while bit < SPAN:
        if r & bit:
            result = result + bit * (1 - 2 * lax.rem(place // bit, 2))
        bit *= 2
    return result


def kernel(
    n_src,
    n_act,
    state_ref,
    mass_ref,
    phase_ref,
    level_ref,
    out_ref,
    own0,
    own1,
    tile_a,
    tile_b,
    got0,
    got1,
    got_act,
    aim0,
    aim1,
    wide,
    columns,
    sums,
    give0,
    give1,
    take0,
    take1,
    line0,
    line1,
    lines0,
    lines1,
    hot,
    held,
    send_sem,
    recv_sem,
    down_sem,
    up_sem,
    block_sem,
    next_ready,
    row_ready,
    act_ready,
):
    n_col = n_src // SPAN
    me = lax.axis_index("src")
    act = lax.axis_index("act")
    group = lax.axis_index("groups")
    place = lax.rem(me, SPAN)
    col = me // SPAN
    base = me - place
    stars = state_ref.shape[1]
    part = stars // n_act
    slots = hot.shape[0]

    col_shift = jnp.where((place == 0) & (act == 0) & (group == 0), 1, 0)
    row_shift = jnp.where((col == 0) & (act == 0) & (group == 0), 1, 0)
    act_shift = jnp.where((me == 0) & (group == 0), 1, 0)
    order = lax.rem(col - col_shift + n_col, n_col)
    row_order = lax.rem(place - row_shift + SPAN, SPAN)
    act_order = lax.rem(act - act_shift + n_act, n_act)

    def ordered(b):
        return {"src": lax.rem(b + col_shift + n_col, n_col) * SPAN + place, "act": act}

    col_peer = [{"src": lax.rem(me + SPAN * q, n_src), "act": act} for q in range(n_col)]
    row_place = [flipped(place, r) for r in range(SPAN)]
    row_peer = [{"src": base + p, "act": act} for p in row_place]
    act_place = [lax.rem(act + i, n_act) for i in range(n_act)]
    act_peer = [{"src": me, "act": a} for a in act_place]
    row_later = [lax.rem(p - row_shift + SPAN, SPAN) > row_order for p in row_place]
    act_later = [lax.rem(a - act_shift + n_act, n_act) > act_order for a in act_place]

    def signal(semaphore, peer):
        pl.semaphore_signal(semaphore, inc=1, device_id=peer, device_id_type=MESH)

    barrier = pltpu.get_barrier_semaphore()

    def greet(b, carry):
        signal(barrier, ordered(b))
        return carry

    lax.fori_loop(order + 1, n_col, greet, 0)
    for later, peers in ((row_later, row_peer), (act_later, act_peer)):
        for k in range(1, len(peers)):
            pl.when(later[k])(functools.partial(signal, barrier, peers[k]))

    counter = [0]

    def exchange(peers, source, target, back, rows=8):
        n = len(peers)
        copies = [None] * n
        for k in range(1, n):
            copies[back(k)] = pltpu.make_async_remote_copy(
                src_ref=source(k),
                dst_ref=target.at[back(k), 0:rows],
                send_sem=send_sem.at[counter[0] + k],
                recv_sem=recv_sem.at[counter[0] + back(k)],
                device_id=peers[k],
                device_id_type=MESH,
            )
        counter[0] += n
        return copies

    def col_back(k):
        return n_col - k

    def row_back(k):
        return k

    def act_back(k):
        return n_act - k

    def block_copy(source, b, semaphore, peer):
        return pltpu.make_async_remote_copy(
            src_ref=source,
            dst_ref=got0.at[b],
            send_sem=semaphore,
            recv_sem=block_sem.at[b],
            device_id=peer,
            device_id_type=MESH,
        )

    def down(b):
        return block_copy(own0, order, down_sem.at[b], ordered(b))

    def up():
        return block_copy(own0, order, up_sem.at[order], ordered(order + 1))

    def pass_up(b):
        return block_copy(got0.at[b], b, up_sem.at[b], ordered(order + 1))

    total = jnp.float32(stars * n_src)
    mine = pl.ds(pl.multiple_of(act * part, part), part)
    level = level_ref[:, mine]
    tick_count = jnp.left_shift(jnp.int32(1), LEVELS - 1 - level).astype(jnp.float32)
    weight = mass_ref[:, mine] / total
    for substep, own in ((0, own0), (1, own1)):
        elapsed = (
            jnp.where(
                level == LEVELS - 1,
                1.0,
                phase_ref[:, mine] * (tick_count - STEPS) + (substep + 1),
            )
            * fine_step
        )
        pos, vel = predict(
            state_ref[0:3, mine],
            state_ref[3:6, mine],
            state_ref[6:9, mine],
            state_ref[9:12, mine],
            elapsed,
        )
        own[0:3, :] = pos
        own[3:6, :] = vel
        own[6:7, :] = weight if substep == 0 else jnp.where(level == LEVELS - 1, 0.0, weight)
        own[7:8, :] = jnp.zeros((1, part), jnp.float32)

    is_active = level_ref[...] == LEVELS - 1
    flags = jnp.broadcast_to(jnp.where(is_active, 1.0, 0.0), (8, stars))
    before = lax.broadcasted_iota(jnp.int32, (stars, stars), 0) < lax.broadcasted_iota(
        jnp.int32, (stars, stars), 1
    )
    rank = jnp.dot(
        flags.astype(jnp.bfloat16),
        jnp.where(before, 1.0, 0.0).astype(jnp.bfloat16),
        preferred_element_type=jnp.float32,
    )[0:1, :]
    rank = jnp.where(is_active, rank, float(slots)).astype(jnp.int32)
    hot[...] = jnp.where(
        lax.broadcasted_iota(jnp.int32, (slots, stars), 0) == rank, 1.0, 0.0
    )
    over_stars = (((1,), (1,)), ((), ()))
    held[0:12, :] = lax.dot_general(
        state_ref[...], hot[...], over_stars, precision=HIGHEST, preferred_element_type=jnp.float32
    )
    held_mass = lax.dot_general(
        jnp.broadcast_to(mass_ref[...] / total, (8, stars)),
        hot[...],
        over_stars,
        precision=HIGHEST,
        preferred_element_type=jnp.float32,
    )[0:1, :]

    def predict_held(tile):
        pos, vel = predict(
            held[0:3, :], held[3:6, :], held[6:9, :], held[9:12, :], fine_step
        )
        tile[0:3, :] = pos
        tile[3:6, :] = vel
        tile[6:7, :] = held_mass
        tile[7:8, :] = jnp.zeros((1, slots), jnp.float32)

    predict_held(tile_a)
    aim0[0] = tile_a[...]

    earlier = order + row_order + act_order
    pl.when(earlier > 0)(lambda: pl.semaphore_wait(barrier, earlier))
    rows0 = exchange(row_peer, lambda k: tile_a, aim0, row_back)
    pl.when(order > 0)(lambda: signal(next_ready, ordered(order - 1)))
    for r in range(1, SPAN):
        pl.when(~row_later[r])(functools.partial(signal, row_ready.at[r], row_peer[r]))
    for i in range(1, n_act):
        pl.when(~act_later[i])(functools.partial(signal, act_ready.at[n_act - i], act_peer[i]))
    far_first = sorted(range(1, n_col), key=lambda q: -min(q, n_col - q))
    near_first = far_first[::-1]
    for q in far_first:
        pl.when(order >= q)(lambda q=q: down(order - q).start())
    for r in range(1, SPAN):
        pl.when(~row_later[r])(lambda r=r: rows0[r].start())
    spread(own0[...], wide.at[0])
    for r in range(1, SPAN):

        @pl.when(row_later[r])
        def _(r=r):
            pl.semaphore_wait(row_ready.at[r], 1)
            rows0[r].start()

    @pl.when(order < n_col - 1)
    def _():
        pl.semaphore_wait(next_ready, 1)
        up().start()

    def over_pairs(source, count, targets, first, lowest=0):
        def one(pair, carry):
            accumulate(source, count, targets, sums, pair, first)
            return carry

        lax.fori_loop(lowest, SPAN // 2, one, 0)

    def last_block(source, count, targets, give, copies):
        for pair in reversed(range(SPAN // 2)):
            accumulate(source, count, targets, sums, pair, False)
            for k in (2 * pair, 2 * pair + 1):
                for row in range(6):
                    give[k, row : row + 1, :] = jnp.sum(sums[k, row], axis=0, keepdims=True)
                if k > 0:
                    copies[k].start()

    def reduced(give, take, copies, line, lines, act_copies, meet):
        for copy in copies[1:]:
            copy.wait_recv()
        summed = give[0, 0:6, :]
        for r in range(1, SPAN):
            summed = summed + take[r, 0:6, :]
        line[0:6, :] = summed
        for copy in act_copies[1:]:
            copy.start()
        meet()
        for copy in act_copies[1:]:
            copy.wait_recv()
        near = [summed] + [lines[i, 0:6, :] for i in range(1, n_act)]
        while len(near) > 1:
            half = len(near) // 2
            near = [near[i] + near[i + half] for i in range(half)]
        return near[0]

    def corrected(forces, tile):
        acc_old, jerk_old = held[6:9, :], held[9:12, :]
        acc_new, jerk_new = forces[0:3, :], forces[3:6, :]
        pos, vel = correct(acc_old, jerk_old, acc_new, jerk_new, tile[0:3, :], tile[3:6, :])
        held[0:3, :] = pos
        held[3:6, :] = vel
        held[6:9, :] = acc_new
        held[9:12, :] = jerk_new

    def wait_block(b):
        block_copy(own0, b, down_sem.at[b], ordered(order + 1)).wait_recv()

    for copy in rows0[1:]:
        copy.wait_recv()
    over_pairs(wide.at[0], part, aim0, True)

    @pl.when(order < n_col - 1)
    def _():
        def forward(j, carry):
            wait_block(order - j)
            pass_up(order - j).start()
            return carry

        lax.fori_loop(1, order + 1, forward, 0)

    def lower(j, carry):
        pl.when(order == n_col - 1)(lambda: wait_block(order - j))
        spread(got0[order - j], wide.at[0])
        over_pairs(wide.at[0], part, aim0, False)
        return carry

    lax.fori_loop(1, jnp.minimum(order, n_col - 2) + 1, lower, 0)

    def upper(b, carry):
        wait_block(b)
        spread(got0[b], wide.at[0])
        over_pairs(wide.at[0], part, aim0, False)
        return carry

    lax.fori_loop(order + 1, n_col - 1, upper, 0)
    for i in range(1, n_act):
        pl.when(act_later[i])(lambda i=i: pl.semaphore_wait(act_ready.at[i], 1))
    gives0 = exchange(row_peer, lambda k: give0.at[k, 0:6], take0, row_back, 6)
    acts0 = exchange(act_peer, lambda k: line0.at[0:6], lines0, act_back, 6)
    cols1 = exchange(col_peer, lambda k: own1, got1, col_back)
    final = jnp.where(order == n_col - 1, 0, n_col - 1)
    wait_block(final)
    spread(got0[final], wide.at[0])
    last_block(wide.at[0], part, aim0, give0, gives0)

    def send_second():
        for q in far_first:
            cols1[n_col - q].start()
        spread(own1[...], wide.at[0])

    corrected(reduced(give0, take0, gives0, line0, lines0, acts0, send_second), tile_a)

    predict_held(tile_b)
    cols2 = exchange(col_peer, lambda k: tile_b, got_act, col_back)
    rows1 = exchange(row_peer, lambda k: tile_b, aim1, row_back)
    cols2[n_col - far_first[0]].start()
    for copy in rows1[1:]:
        copy.start()
    for q in far_first[1:]:
        cols2[n_col - q].start()
    aim1[0] = tile_b[...]
    share = slots // n_act
    first_slot = act * share
    spread_part(tile_b[...], columns, first_slot, share, wide.at[1], 0)
    rows1[1].wait_recv()
    accumulate(wide.at[0], part, aim1, sums, 0, True)
    for n, q in enumerate(near_first[:2]):
        cols1[q].wait_recv()
        spread(got1[q], wide.at[2 + n])
        accumulate(wide.at[2 + n], part, aim1, sums, 0, False)
    for copy in rows1[2:]:
        copy.wait_recv()
    over_pairs(wide.at[0], part, aim1, True, 1)
    over_pairs(wide.at[2], part, aim1, False, 1)
    over_pairs(wide.at[3], part, aim1, False, 1)
    for q in near_first[2:]:
        cols1[q].wait_recv()
        spread(got1[q], wide.at[0])
        over_pairs(wide.at[0], part, aim1, False)
    gives1 = exchange(row_peer, lambda k: give1.at[k, 0:6], take1, row_back, 6)
    acts1 = exchange(act_peer, lambda k: line1.at[0:6], lines1, act_back, 6)
    for n, q in enumerate(near_first[:-1]):
        cols2[q].wait_recv()
        spread_part(got_act[q], columns, first_slot, share, wide.at[1], (n + 1) * share)
    over_pairs(wide.at[1], (n_col - 1) * share, aim1, False)
    cols2[near_first[-1]].wait_recv()
    spread_part(got_act[near_first[-1]], columns, first_slot, share, wide.at[2], 0)
    last_block(wide.at[2], share, aim1, give1, gives1)
    corrected(reduced(give1, take1, gives1, line1, lines1, acts1, lambda: None), tile_b)

    moved = jnp.dot(held[...], hot[...], precision=HIGHEST, preferred_element_type=jnp.float32)
    out_ref[...] = jnp.where(is_active, moved[0:12, :], state_ref[...])
    for copies in (rows0, cols1, gives0, acts0, cols2, rows1, gives1, acts1):
        for copy in copies[1:]:
            copy.wait_send()

    def down_sent(b, carry):
        down(b).wait_send()
        return carry

    lax.fori_loop(0, order, down_sent, 0)

    @pl.when(order < n_col - 1)
    def _():
        up().wait_send()

        def up_sent(b, carry):
            pass_up(b).wait_send()
            return carry

        lax.fori_loop(0, order, up_sent, 0)


def solution(mesh):
    n_src, n_act = mesh.shape["src"], mesh.shape["act"]
    n_col = n_src // SPAN

    def per_device(star_state, masses, phases, levels, active_list, active_count):
        stars = star_state.shape[1]
        part = stars // n_act
        slots = 2 * active_list.shape[0]
        vmem = pl.BlockSpec(memory_space=pltpu.VMEM)
        n_sem = 2 * n_col + 4 * SPAN + 2 * n_act

        def tiles(*lead):
            return pltpu.VMEM((*lead, 8, 128), jnp.float32)

        return pl.pallas_call(
            functools.partial(kernel, n_src, n_act),
            out_shape=jax.ShapeDtypeStruct(star_state.shape, jnp.float32),
            in_specs=[vmem] * 4,
            out_specs=vmem,
            scratch_shapes=[
                pltpu.VMEM((8, part), jnp.float32),
                pltpu.VMEM((8, part), jnp.float32),
                pltpu.VMEM((8, slots), jnp.float32),
                pltpu.VMEM((8, slots), jnp.float32),
                pltpu.VMEM((n_col, 8, part), jnp.float32),
                pltpu.VMEM((n_col, 8, part), jnp.float32),
                pltpu.VMEM((n_col, 8, slots), jnp.float32),
                pltpu.VMEM((SPAN, 8, slots), jnp.float32),
                pltpu.VMEM((SPAN, 8, slots), jnp.float32),
                pltpu.VMEM((4, 7, max(part, n_col * slots // n_act), 128), jnp.float32),
                pltpu.VMEM((slots, 8), jnp.float32),
                tiles(SPAN, 6),
                tiles(SPAN),
                tiles(SPAN),
                tiles(SPAN),
                tiles(SPAN),
                tiles(),
                tiles(),
                tiles(n_act),
                tiles(n_act),
                pltpu.VMEM((slots, stars), jnp.float32),
                pltpu.VMEM((12, slots), jnp.float32),
                pltpu.SemaphoreType.DMA((n_sem,)),
                pltpu.SemaphoreType.DMA((n_sem,)),
                pltpu.SemaphoreType.DMA((n_col,)),
                pltpu.SemaphoreType.DMA((n_col,)),
                pltpu.SemaphoreType.DMA((n_col,)),
                pltpu.SemaphoreType.REGULAR,
                pltpu.SemaphoreType.REGULAR((SPAN,)),
                pltpu.SemaphoreType.REGULAR((n_act,)),
            ],
            compiler_params=pltpu.CompilerParams(collective_id=0, has_side_effects=True),
        )(
            star_state,
            masses.reshape(1, stars),
            phases.reshape(1, stars),
            levels.reshape(1, stars),
        )

    in_specs = (
        P(None, ("groups", "src")),
        P(("groups", "src")),
        P(("groups", "src")),
        P(("groups", "src")),
        P(("groups", "src", "act")),
        P(("groups", "src", "act")),
    )
    return jax.shard_map(
        per_device,
        mesh=mesh,
        in_specs=in_specs,
        out_specs=P(None, ("groups", "src")),
        check_vma=False,
    )
```

```python
import functools

import jax
import jax.numpy as jnp
from jax import lax
from jax.experimental import pallas as pl
from jax.experimental.pallas import tpu as pltpu
from jax.sharding import PartitionSpec as P

LEVELS = 5
STEPS = 2
SPAN = 8

soften_sq = 0.0004
fine_step = 0.03125
MESH = pl.DeviceIdType.MESH
HIGHEST = lax.Precision.HIGHEST


def predict(pos, vel, acc, jerk, interval):
    new_pos = pos + interval * (vel + interval * (0.5 * acc + interval * jerk / 6.0))
    new_vel = vel + interval * (acc + 0.5 * interval * jerk)
    return new_pos, new_vel


def correct(acc_old, jerk_old, acc_new, jerk_new, pos_pred, vel_pred):
    snap_term = (-6.0 * (acc_old - acc_new) - fine_step * (4.0 * jerk_old + 2.0 * jerk_new)) / (
        fine_step * fine_step
    )
    crackle = (12.0 * (acc_old - acc_new) + 6.0 * fine_step * (jerk_old + jerk_new)) / (
        fine_step * fine_step * fine_step
    )
    pos = pos_pred + fine_step**4 / 24.0 * snap_term + fine_step**5 / 120.0 * crackle
    vel = vel_pred + fine_step**3 / 6.0 * snap_term + fine_step**4 / 24.0 * crackle
    return pos, vel


def spread(tile, wide):
    stars = tile.shape[1]
    columns = jnp.transpose(tile)
    for row in range(7):
        wide[row, 0:stars, :] = jnp.broadcast_to(columns[:, row : row + 1], (stars, 128))


def spread_part(tile, columns, begin, count, wide, at):
    columns[...] = jnp.transpose(tile)
    chosen = columns[pl.ds(pl.multiple_of(begin, count), count), :]
    for row in range(7):
        wide[row, at : at + count, :] = jnp.broadcast_to(chosen[:, row : row + 1], (count, 128))


def accumulate(wide, count, targets, sums, pair, first):
    aim = [
        [jnp.broadcast_to(targets[2 * pair + i, row : row + 1, :], (8, 128)) for row in range(6)]
        for i in range(2)
    ]

    def body(step, totals):
        rows = pl.ds(pl.multiple_of(step * 8, 8), 8)
        source = [wide[row, rows, :] for row in range(7)]
        finished = []
        for i in range(2):
            dx, dy, dz, du, dv, dw = [source[row] - aim[i][row] for row in range(6)]
            dist_sq = dx * dx + dy * dy + dz * dz + soften_sq
            inverse = lax.rsqrt(dist_sq)
            inv_sq = inverse * inverse
            weight = source[6] * inverse * inv_sq
            radial = (dx * du + dy * dv + dz * dw) * inv_sq * 3.0
            part = [weight * d for d in (dx, dy, dz)]
            part += [weight * (e - radial * d) for d, e in ((dx, du), (dy, dv), (dz, dw))]
            finished += part
        return tuple(t + p for t, p in zip(totals, finished))

    if first:
        totals = tuple(jnp.zeros((8, 128), jnp.float32) for _ in range(12))
    else:
        totals = tuple(sums[2 * pair + i, row] for i in range(2) for row in range(6))
    totals = lax.fori_loop(0, count // 8, body, totals, unroll=2)
    for i in range(2):
        for row in range(6):
            sums[2 * pair + i, row] = totals[6 * i + row]


def flipped(place, r):
    result, bit = place, 1
    while bit < SPAN:
        if r & bit:
            result = result + bit * (1 - 2 * lax.rem(place // bit, 2))
        bit *= 2
    return result


def kernel(
    n_src,
    n_act,
    state_in,
    mass_in,
    phase_in,
    level_in,
    out_ref,
    state_ref,
    mass_ref,
    phase_ref,
    level_ref,
    in_sem,
    own0,
    own1,
    tile_a,
    tile_b,
    got0,
    got1,
    got_act,
    aim0,
    aim1,
    wide,
    columns,
    sums,
    give0,
    give1,
    take0,
    take1,
    line0,
    line1,
    lines0,
    lines1,
    hot,
    held,
    send_sem,
    recv_sem,
    down_sem,
    up_sem,
    block_sem,
    next_ready,
    row_ready,
    act_ready,
):
    loads = [
        pltpu.make_async_copy(source, target, in_sem.at[k])
        for k, (source, target) in enumerate(
            (
                (state_in, state_ref),
                (mass_in, mass_ref),
                (phase_in, phase_ref),
                (level_in, level_ref),
            )
        )
    ]
    for load in loads:
        load.start()
    n_col = n_src // SPAN
    me = lax.axis_index("src")
    act = lax.axis_index("act")
    group = lax.axis_index("groups")
    place = lax.rem(me, SPAN)
    col = me // SPAN
    base = me - place
    stars = state_ref.shape[1]
    part = stars // n_act
    slots = hot.shape[0]

    col_shift = jnp.where((place == 0) & (act == 0) & (group == 0), 1, 0)
    row_shift = jnp.where((col == 0) & (act == 0) & (group == 0), 1, 0)
    act_shift = jnp.where((me == 0) & (group == 0), 1, 0)
    order = lax.rem(col - col_shift + n_col, n_col)
    row_order = lax.rem(place - row_shift + SPAN, SPAN)
    act_order = lax.rem(act - act_shift + n_act, n_act)

    def ordered(b):
        return {"src": lax.rem(b + col_shift + n_col, n_col) * SPAN + place, "act": act}

    col_peer = [{"src": lax.rem(me + SPAN * q, n_src), "act": act} for q in range(n_col)]
    row_place = [flipped(place, r) for r in range(SPAN)]
    row_peer = [{"src": base + p, "act": act} for p in row_place]
    act_place = [lax.rem(act + i, n_act) for i in range(n_act)]
    act_peer = [{"src": me, "act": a} for a in act_place]
    row_later = [lax.rem(p - row_shift + SPAN, SPAN) > row_order for p in row_place]
    act_later = [lax.rem(a - act_shift + n_act, n_act) > act_order for a in act_place]

    def signal(semaphore, peer):
        pl.semaphore_signal(semaphore, inc=1, device_id=peer, device_id_type=MESH)

    barrier = pltpu.get_barrier_semaphore()

    def greet(b, carry):
        signal(barrier, ordered(b))
        return carry

    lax.fori_loop(order + 1, n_col, greet, 0)
    for later, peers in ((row_later, row_peer), (act_later, act_peer)):
        for k in range(1, len(peers)):
            pl.when(later[k])(functools.partial(signal, barrier, peers[k]))

    counter = [0]

    def exchange(peers, source, target, back, rows=8):
        n = len(peers)
        copies = [None] * n
        for k in range(1, n):
            copies[back(k)] = pltpu.make_async_remote_copy(
                src_ref=source(k),
                dst_ref=target.at[back(k), 0:rows],
                send_sem=send_sem.at[counter[0] + k],
                recv_sem=recv_sem.at[counter[0] + back(k)],
                device_id=peers[k],
                device_id_type=MESH,
            )
        counter[0] += n
        return copies

    def col_back(k):
        return n_col - k

    def row_back(k):
        return k

    def act_back(k):
        return n_act - k

    def block_copy(source, b, semaphore, peer):
        return pltpu.make_async_remote_copy(
            src_ref=source,
            dst_ref=got0.at[b],
            send_sem=semaphore,
            recv_sem=block_sem.at[b],
            device_id=peer,
            device_id_type=MESH,
        )

    def down(b):
        return block_copy(own0, order, down_sem.at[b], ordered(b))

    def up():
        return block_copy(own0, order, up_sem.at[order], ordered(order + 1))

    def pass_up(b):
        return block_copy(got0.at[b], b, up_sem.at[b], ordered(order + 1))

    earlier = order + row_order + act_order
    pl.when(earlier > 0)(lambda: pl.semaphore_wait(barrier, earlier))
    rows0 = exchange(row_peer, lambda k: tile_a, aim0, row_back)
    pl.when(order > 0)(lambda: signal(next_ready, ordered(order - 1)))
    for r in range(1, SPAN):
        pl.when(~row_later[r])(functools.partial(signal, row_ready.at[r], row_peer[r]))
    for i in range(1, n_act):
        pl.when(~act_later[i])(functools.partial(signal, act_ready.at[n_act - i], act_peer[i]))

    for load in loads:
        load.wait()
    total = jnp.float32(stars * n_src)
    mine = pl.ds(pl.multiple_of(act * part, part), part)
    level = level_ref[:, mine]
    tick_count = jnp.left_shift(jnp.int32(1), LEVELS - 1 - level).astype(jnp.float32)
    weight = mass_ref[:, mine] / total

    def predict_own(substep, own):
        elapsed = (
            jnp.where(
                level == LEVELS - 1,
                1.0,
                phase_ref[:, mine] * (tick_count - STEPS) + (substep + 1),
            )
            * fine_step
        )
        pos, vel = predict(
            state_ref[0:3, mine],
            state_ref[3:6, mine],
            state_ref[6:9, mine],
            state_ref[9:12, mine],
            elapsed,
        )
        own[0:3, :] = pos
        own[3:6, :] = vel
        own[6:7, :] = weight if substep == 0 else jnp.where(level == LEVELS - 1, 0.0, weight)
        own[7:8, :] = jnp.zeros((1, part), jnp.float32)

    predict_own(0, own0)
    far_first = sorted(range(1, n_col), key=lambda q: -min(q, n_col - q))
    near_first = far_first[::-1]
    for q in far_first:
        pl.when(order >= q)(lambda q=q: down(order - q).start())

    predict_own(1, own1)
    is_active = level_ref[...] == LEVELS - 1
    flags = jnp.broadcast_to(jnp.where(is_active, 1.0, 0.0), (8, stars))
    before = lax.broadcasted_iota(jnp.int32, (stars, stars), 0) < lax.broadcasted_iota(
        jnp.int32, (stars, stars), 1
    )
    rank = jnp.dot(
        flags.astype(jnp.bfloat16),
        jnp.where(before, 1.0, 0.0).astype(jnp.bfloat16),
        preferred_element_type=jnp.float32,
    )[0:1, :]
    rank = jnp.where(is_active, rank, float(slots)).astype(jnp.int32)
    hot[...] = jnp.where(
        lax.broadcasted_iota(jnp.int32, (slots, stars), 0) == rank, 1.0, 0.0
    )
    over_stars = (((1,), (1,)), ((), ()))
    held[0:12, :] = lax.dot_general(
        state_ref[...], hot[...], over_stars, precision=HIGHEST, preferred_element_type=jnp.float32
    )
    held_mass = lax.dot_general(
        jnp.broadcast_to(mass_ref[...] / total, (8, stars)),
        hot[...],
        over_stars,
        precision=HIGHEST,
        preferred_element_type=jnp.float32,
    )[0:1, :]

    def predict_held(tile):
        pos, vel = predict(
            held[0:3, :], held[3:6, :], held[6:9, :], held[9:12, :], fine_step
        )
        tile[0:3, :] = pos
        tile[3:6, :] = vel
        tile[6:7, :] = held_mass
        tile[7:8, :] = jnp.zeros((1, slots), jnp.float32)

    predict_held(tile_a)
    aim0[0] = tile_a[...]

    for r in range(1, SPAN):
        pl.when(~row_later[r])(lambda r=r: rows0[r].start())
    spread(own0[...], wide.at[0])
    def answer_row():
        for r in range(1, SPAN):

            @pl.when(row_later[r])
            def _(r=r):
                pl.semaphore_wait(row_ready.at[r], 1)
                rows0[r].start()

    pl.when(row_shift == 0)(answer_row)

    @pl.when(order < n_col - 1)
    def _():
        pl.semaphore_wait(next_ready, 1)
        up().start()

    pl.when(row_shift == 1)(answer_row)

    def over_pairs(source, count, targets, first, lowest=0):
        def one(pair, carry):
            accumulate(source, count, targets, sums, pair, first)
            return carry

        lax.fori_loop(lowest, SPAN // 2, one, 0)

    def last_block(source, count, targets, give, copies):
        for pair in reversed(range(SPAN // 2)):
            accumulate(source, count, targets, sums, pair, False)
            for k in (2 * pair, 2 * pair + 1):
                for row in range(6):
                    give[k, row : row + 1, :] = jnp.sum(sums[k, row], axis=0, keepdims=True)
                if k > 0:
                    copies[k].start()

    def reduced(give, take, copies, line, lines, act_copies, meet):
        for copy in copies[1:]:
            copy.wait_recv()
        summed = give[0, 0:6, :]
        for r in range(1, SPAN):
            summed = summed + take[r, 0:6, :]
        line[0:6, :] = summed
        for copy in act_copies[1:]:
            copy.start()
        meet()
        for copy in act_copies[1:]:
            copy.wait_recv()
        near = [summed] + [lines[i, 0:6, :] for i in range(1, n_act)]
        while len(near) > 1:
            half = len(near) // 2
            near = [near[i] + near[i + half] for i in range(half)]
        return near[0]

    def corrected(forces, tile):
        acc_old, jerk_old = held[6:9, :], held[9:12, :]
        acc_new, jerk_new = forces[0:3, :], forces[3:6, :]
        pos, vel = correct(acc_old, jerk_old, acc_new, jerk_new, tile[0:3, :], tile[3:6, :])
        held[0:3, :] = pos
        held[3:6, :] = vel
        held[6:9, :] = acc_new
        held[9:12, :] = jerk_new

    def wait_block(b):
        block_copy(own0, b, down_sem.at[b], ordered(order + 1)).wait_recv()

    for copy in rows0[1:]:
        copy.wait_recv()
    over_pairs(wide.at[0], part, aim0, True)

    @pl.when(order < n_col - 1)
    def _():
        def forward(j, carry):
            wait_block(order - j)
            pass_up(order - j).start()
            return carry

        lax.fori_loop(1, order + 1, forward, 0)

    def lower(j, carry):
        pl.when(order == n_col - 1)(lambda: wait_block(order - j))
        spread(got0[order - j], wide.at[0])
        over_pairs(wide.at[0], part, aim0, False)
        return carry

    lax.fori_loop(1, jnp.minimum(order, n_col - 2) + 1, lower, 0)

    def upper(b, carry):
        wait_block(b)
        spread(got0[b], wide.at[0])
        over_pairs(wide.at[0], part, aim0, False)
        return carry

    lax.fori_loop(order + 1, n_col - 1, upper, 0)
    for i in range(1, n_act):
        pl.when(act_later[i])(lambda i=i: pl.semaphore_wait(act_ready.at[i], 1))
    gives0 = exchange(row_peer, lambda k: give0.at[k, 0:6], take0, row_back, 6)
    acts0 = exchange(act_peer, lambda k: line0.at[0:6], lines0, act_back, 6)
    cols1 = exchange(col_peer, lambda k: own1, got1, col_back)
    final = jnp.where(order == n_col - 1, 0, n_col - 1)
    wait_block(final)
    spread(got0[final], wide.at[0])
    last_block(wide.at[0], part, aim0, give0, gives0)

    def send_second():
        for q in far_first:
            cols1[n_col - q].start()
        spread(own1[...], wide.at[0])

    corrected(reduced(give0, take0, gives0, line0, lines0, acts0, send_second), tile_a)

    predict_held(tile_b)
    cols2 = exchange(col_peer, lambda k: tile_b, got_act, col_back)
    rows1 = exchange(row_peer, lambda k: tile_b, aim1, row_back)
    cols2[n_col - far_first[0]].start()
    for copy in rows1[1:]:
        copy.start()
    for q in far_first[1:]:
        cols2[n_col - q].start()
    aim1[0] = tile_b[...]
    share = slots // n_act
    first_slot = act * share
    spread_part(tile_b[...], columns, first_slot, share, wide.at[1], 0)
    rows1[1].wait_recv()
    accumulate(wide.at[0], part, aim1, sums, 0, True)
    for n, q in enumerate(near_first[:2]):
        cols1[q].wait_recv()
        spread(got1[q], wide.at[2 + n])
        accumulate(wide.at[2 + n], part, aim1, sums, 0, False)
    for copy in rows1[2:]:
        copy.wait_recv()
    over_pairs(wide.at[0], part, aim1, True, 1)
    over_pairs(wide.at[2], part, aim1, False, 1)
    over_pairs(wide.at[3], part, aim1, False, 1)
    for q in near_first[2:]:
        cols1[q].wait_recv()
        spread(got1[q], wide.at[0])
        over_pairs(wide.at[0], part, aim1, False)
    gives1 = exchange(row_peer, lambda k: give1.at[k, 0:6], take1, row_back, 6)
    acts1 = exchange(act_peer, lambda k: line1.at[0:6], lines1, act_back, 6)
    for n, q in enumerate(near_first[:-1]):
        cols2[q].wait_recv()
        spread_part(got_act[q], columns, first_slot, share, wide.at[1], (n + 1) * share)
    over_pairs(wide.at[1], (n_col - 1) * share, aim1, False)
    cols2[near_first[-1]].wait_recv()
    spread_part(got_act[near_first[-1]], columns, first_slot, share, wide.at[2], 0)
    last_block(wide.at[2], share, aim1, give1, gives1)
    corrected(reduced(give1, take1, gives1, line1, lines1, acts1, lambda: None), tile_b)

    moved = jnp.dot(held[...], hot[...], precision=HIGHEST, preferred_element_type=jnp.float32)
    out_ref[...] = jnp.where(is_active, moved[0:12, :], state_ref[...])
    for copies in (rows0, cols1, gives0, acts0, cols2, rows1, gives1, acts1):
        for copy in copies[1:]:
            copy.wait_send()

    def down_sent(b, carry):
        down(b).wait_send()
        return carry

    lax.fori_loop(0, order, down_sent, 0)

    @pl.when(order < n_col - 1)
    def _():
        up().wait_send()

        def up_sent(b, carry):
            pass_up(b).wait_send()
            return carry

        lax.fori_loop(0, order, up_sent, 0)


def solution(mesh):
    n_src, n_act = mesh.shape["src"], mesh.shape["act"]
    n_col = n_src // SPAN

    def per_device(star_state, masses, phases, levels, active_list, active_count):
        stars = star_state.shape[1]
        part = stars // n_act
        slots = 2 * active_list.shape[0]
        vmem = pl.BlockSpec(memory_space=pltpu.VMEM)
        n_sem = 2 * n_col + 4 * SPAN + 2 * n_act

        def tiles(*lead):
            return pltpu.VMEM((*lead, 8, 128), jnp.float32)

        return pl.pallas_call(
            functools.partial(kernel, n_src, n_act),
            out_shape=jax.ShapeDtypeStruct(star_state.shape, jnp.float32),
            in_specs=[pl.BlockSpec(memory_space=pl.ANY)] * 4,
            out_specs=vmem,
            scratch_shapes=[
                pltpu.VMEM(star_state.shape, jnp.float32),
                pltpu.VMEM((1, stars), jnp.float32),
                pltpu.VMEM((1, stars), jnp.float32),
                pltpu.VMEM((1, stars), jnp.int32),
                pltpu.SemaphoreType.DMA((4,)),
                pltpu.VMEM((8, part), jnp.float32),
                pltpu.VMEM((8, part), jnp.float32),
                pltpu.VMEM((8, slots), jnp.float32),
                pltpu.VMEM((8, slots), jnp.float32),
                pltpu.VMEM((n_col, 8, part), jnp.float32),
                pltpu.VMEM((n_col, 8, part), jnp.float32),
                pltpu.VMEM((n_col, 8, slots), jnp.float32),
                pltpu.VMEM((SPAN, 8, slots), jnp.float32),
                pltpu.VMEM((SPAN, 8, slots), jnp.float32),
                pltpu.VMEM((4, 7, max(part, n_col * slots // n_act), 128), jnp.float32),
                pltpu.VMEM((slots, 8), jnp.float32),
                tiles(SPAN, 6),
                tiles(SPAN),
                tiles(SPAN),
                tiles(SPAN),
                tiles(SPAN),
                tiles(),
                tiles(),
                tiles(n_act),
                tiles(n_act),
                pltpu.VMEM((slots, stars), jnp.float32),
                pltpu.VMEM((12, slots), jnp.float32),
                pltpu.SemaphoreType.DMA((n_sem,)),
                pltpu.SemaphoreType.DMA((n_sem,)),
                pltpu.SemaphoreType.DMA((n_col,)),
                pltpu.SemaphoreType.DMA((n_col,)),
                pltpu.SemaphoreType.DMA((n_col,)),
                pltpu.SemaphoreType.REGULAR,
                pltpu.SemaphoreType.REGULAR((SPAN,)),
                pltpu.SemaphoreType.REGULAR((n_act,)),
            ],
            compiler_params=pltpu.CompilerParams(collective_id=0, has_side_effects=True),
        )(
            star_state,
            masses.reshape(1, stars),
            phases.reshape(1, stars),
            levels.reshape(1, stars),
        )

    in_specs = (
        P(None, ("groups", "src")),
        P(("groups", "src")),
        P(("groups", "src")),
        P(("groups", "src")),
        P(("groups", "src", "act")),
        P(("groups", "src", "act")),
    )
    return jax.shard_map(
        per_device,
        mesh=mesh,
        in_specs=in_specs,
        out_specs=P(None, ("groups", "src")),
        check_vma=False,
    )
```

```python
import functools

import jax
import jax.numpy as jnp
from jax import lax
from jax.experimental import pallas as pl
from jax.experimental.pallas import tpu as pltpu
from jax.sharding import PartitionSpec as P

LEVELS = 5
STEPS = 2
SPAN = 8

soften_sq = 0.0004
fine_step = 0.03125
MESH = pl.DeviceIdType.MESH
HIGHEST = lax.Precision.HIGHEST


def predict(pos, vel, acc, jerk, interval):
    new_pos = pos + interval * (vel + interval * (0.5 * acc + interval * jerk / 6.0))
    new_vel = vel + interval * (acc + 0.5 * interval * jerk)
    return new_pos, new_vel


def correct(acc_old, jerk_old, acc_new, jerk_new, pos_pred, vel_pred):
    snap_term = (-6.0 * (acc_old - acc_new) - fine_step * (4.0 * jerk_old + 2.0 * jerk_new)) / (
        fine_step * fine_step
    )
    crackle = (12.0 * (acc_old - acc_new) + 6.0 * fine_step * (jerk_old + jerk_new)) / (
        fine_step * fine_step * fine_step
    )
    pos = pos_pred + fine_step**4 / 24.0 * snap_term + fine_step**5 / 120.0 * crackle
    vel = vel_pred + fine_step**3 / 6.0 * snap_term + fine_step**4 / 24.0 * crackle
    return pos, vel


def spread(tile, wide):
    stars = tile.shape[1]
    columns = jnp.transpose(tile)
    for row in range(7):
        wide[row, 0:stars, :] = jnp.broadcast_to(columns[:, row : row + 1], (stars, 128))


def spread_part(tile, columns, begin, count, wide, at):
    columns[...] = jnp.transpose(tile)
    chosen = columns[pl.ds(pl.multiple_of(begin, count), count), :]
    for row in range(7):
        wide[row, at : at + count, :] = jnp.broadcast_to(chosen[:, row : row + 1], (count, 128))


def accumulate(wide, count, targets, sums, pair, first):
    aim = [
        [jnp.broadcast_to(targets[2 * pair + i, row : row + 1, :], (8, 128)) for row in range(6)]
        for i in range(2)
    ]

    def body(step, totals):
        rows = pl.ds(pl.multiple_of(step * 8, 8), 8)
        source = [wide[row, rows, :] for row in range(7)]
        finished = []
        for i in range(2):
            dx, dy, dz, du, dv, dw = [source[row] - aim[i][row] for row in range(6)]
            dist_sq = dx * dx + dy * dy + dz * dz + soften_sq
            inverse = lax.rsqrt(dist_sq)
            inv_sq = inverse * inverse
            weight = source[6] * inverse * inv_sq
            radial = (dx * du + dy * dv + dz * dw) * inv_sq * 3.0
            part = [weight * d for d in (dx, dy, dz)]
            part += [weight * (e - radial * d) for d, e in ((dx, du), (dy, dv), (dz, dw))]
            finished += part
        return tuple(t + p for t, p in zip(totals, finished))

    if first:
        totals = tuple(jnp.zeros((8, 128), jnp.float32) for _ in range(12))
    else:
        totals = tuple(sums[2 * pair + i, row] for i in range(2) for row in range(6))
    totals = lax.fori_loop(0, count // 8, body, totals, unroll=2)
    for i in range(2):
        for row in range(6):
            sums[2 * pair + i, row] = totals[6 * i + row]


def flipped(place, r):
    result, bit = place, 1
    while bit < SPAN:
        if r & bit:
            result = result + bit * (1 - 2 * lax.rem(place // bit, 2))
        bit *= 2
    return result


def kernel(
    n_src,
    n_act,
    state_in,
    mass_in,
    phase_in,
    level_in,
    out_ref,
    state_ref,
    mass_ref,
    phase_ref,
    level_ref,
    in_sem,
    own0,
    own1,
    tile_a,
    tile_b,
    got0,
    got1,
    got_act,
    aim0,
    aim1,
    wide,
    columns,
    sums,
    give0,
    give1,
    take0,
    take1,
    line0,
    line1,
    lines0,
    lines1,
    hot,
    held,
    send_sem,
    recv_sem,
    down_sem,
    up_sem,
    block_sem,
    next_ready,
    row_ready,
    act_ready,
    wrap_sem,
    wrap_ready,
):
    loads = [
        pltpu.make_async_copy(source, target, in_sem.at[k])
        for k, (source, target) in enumerate(
            (
                (state_in, state_ref),
                (mass_in, mass_ref),
                (phase_in, phase_ref),
                (level_in, level_ref),
            )
        )
    ]
    for load in loads:
        load.start()
    n_col = n_src // SPAN
    me = lax.axis_index("src")
    act = lax.axis_index("act")
    group = lax.axis_index("groups")
    place = lax.rem(me, SPAN)
    col = me // SPAN
    base = me - place
    stars = state_ref.shape[1]
    part = stars // n_act
    slots = hot.shape[0]

    col_shift = jnp.where((place == 0) & (act == 0) & (group == 0), 1, 0)
    row_shift = jnp.where((col == 0) & (act == 0) & (group == 0), 1, 0)
    act_shift = jnp.where((me == 0) & (group == 0), 1, 0)
    order = lax.rem(col - col_shift + n_col, n_col)
    row_order = lax.rem(place - row_shift + SPAN, SPAN)
    act_order = lax.rem(act - act_shift + n_act, n_act)

    def ordered(b):
        return {"src": lax.rem(b + col_shift + n_col, n_col) * SPAN + place, "act": act}

    col_peer = [{"src": lax.rem(me + SPAN * q, n_src), "act": act} for q in range(n_col)]
    row_place = [flipped(place, r) for r in range(SPAN)]
    row_peer = [{"src": base + p, "act": act} for p in row_place]
    act_place = [lax.rem(act + i, n_act) for i in range(n_act)]
    act_peer = [{"src": me, "act": a} for a in act_place]
    row_later = [lax.rem(p - row_shift + SPAN, SPAN) > row_order for p in row_place]
    act_later = [lax.rem(a - act_shift + n_act, n_act) > act_order for a in act_place]

    def signal(semaphore, peer):
        pl.semaphore_signal(semaphore, inc=1, device_id=peer, device_id_type=MESH)

    barrier = pltpu.get_barrier_semaphore()

    def greet(b, carry):
        signal(barrier, ordered(b))
        return carry

    lax.fori_loop(order + 1, n_col, greet, 0)
    for later, peers in ((row_later, row_peer), (act_later, act_peer)):
        for k in range(1, len(peers)):
            pl.when(later[k])(functools.partial(signal, barrier, peers[k]))

    counter = [0]

    def exchange(peers, source, target, back, rows=8):
        n = len(peers)
        copies = [None] * n
        for k in range(1, n):
            copies[back(k)] = pltpu.make_async_remote_copy(
                src_ref=source(k),
                dst_ref=target.at[back(k), 0:rows],
                send_sem=send_sem.at[counter[0] + k],
                recv_sem=recv_sem.at[counter[0] + back(k)],
                device_id=peers[k],
                device_id_type=MESH,
            )
        counter[0] += n
        return copies

    def col_back(k):
        return n_col - k

    def row_back(k):
        return k

    def act_back(k):
        return n_act - k

    def block_copy(source, b, semaphore, peer):
        return pltpu.make_async_remote_copy(
            src_ref=source,
            dst_ref=got0.at[b],
            send_sem=semaphore,
            recv_sem=block_sem.at[b],
            device_id=peer,
            device_id_type=MESH,
        )

    def down(b):
        return block_copy(own0, order, down_sem.at[b], ordered(b))

    def up():
        return block_copy(own0, order, up_sem.at[order], ordered(order + 1))

    def pass_up(b):
        return block_copy(got0.at[b], b, up_sem.at[b], ordered(order + 1))

    earlier = order + row_order + act_order
    pl.when(earlier > 0)(lambda: pl.semaphore_wait(barrier, earlier))
    rows0 = exchange(row_peer, lambda k: tile_a, aim0, row_back)
    pl.when(order > 0)(lambda: signal(next_ready, ordered(order - 1)))
    for t in range(2):
        pl.when(order == n_col - 2 + t)(lambda t=t: signal(wrap_ready.at[t], ordered(0)))
    for r in range(1, SPAN):
        pl.when(~row_later[r])(functools.partial(signal, row_ready.at[r], row_peer[r]))
    for i in range(1, n_act):
        pl.when(~act_later[i])(functools.partial(signal, act_ready.at[n_act - i], act_peer[i]))

    for load in loads:
        load.wait()
    total = jnp.float32(stars * n_src)
    mine = pl.ds(pl.multiple_of(act * part, part), part)
    level = level_ref[:, mine]
    tick_count = jnp.left_shift(jnp.int32(1), LEVELS - 1 - level).astype(jnp.float32)
    weight = mass_ref[:, mine] / total

    def predict_own(substep, own):
        elapsed = (
            jnp.where(
                level == LEVELS - 1,
                1.0,
                phase_ref[:, mine] * (tick_count - STEPS) + (substep + 1),
            )
            * fine_step
        )
        pos, vel = predict(
            state_ref[0:3, mine],
            state_ref[3:6, mine],
            state_ref[6:9, mine],
            state_ref[9:12, mine],
            elapsed,
        )
        own[0:3, :] = pos
        own[3:6, :] = vel
        own[6:7, :] = weight if substep == 0 else jnp.where(level == LEVELS - 1, 0.0, weight)
        own[7:8, :] = jnp.zeros((1, part), jnp.float32)

    predict_own(0, own0)
    far_first = sorted(range(1, n_col), key=lambda q: -min(q, n_col - q))
    near_first = far_first[::-1]
    for q in far_first:
        pl.when(order >= q)(lambda q=q: down(order - q).start())

    predict_own(1, own1)
    is_active = level_ref[...] == LEVELS - 1
    flags = jnp.broadcast_to(jnp.where(is_active, 1.0, 0.0), (8, stars))
    before = lax.broadcasted_iota(jnp.int32, (stars, stars), 0) < lax.broadcasted_iota(
        jnp.int32, (stars, stars), 1
    )
    rank = jnp.dot(
        flags.astype(jnp.bfloat16),
        jnp.where(before, 1.0, 0.0).astype(jnp.bfloat16),
        preferred_element_type=jnp.float32,
    )[0:1, :]
    rank = jnp.where(is_active, rank, float(slots)).astype(jnp.int32)
    hot[...] = jnp.where(
        lax.broadcasted_iota(jnp.int32, (slots, stars), 0) == rank, 1.0, 0.0
    )
    over_stars = (((1,), (1,)), ((), ()))
    held[0:12, :] = lax.dot_general(
        state_ref[...], hot[...], over_stars, precision=HIGHEST, preferred_element_type=jnp.float32
    )
    held_mass = lax.dot_general(
        jnp.broadcast_to(mass_ref[...] / total, (8, stars)),
        hot[...],
        over_stars,
        precision=HIGHEST,
        preferred_element_type=jnp.float32,
    )[0:1, :]

    def predict_held(tile):
        pos, vel = predict(
            held[0:3, :], held[3:6, :], held[6:9, :], held[9:12, :], fine_step
        )
        tile[0:3, :] = pos
        tile[3:6, :] = vel
        tile[6:7, :] = held_mass
        tile[7:8, :] = jnp.zeros((1, slots), jnp.float32)

    predict_held(tile_a)
    aim0[0] = tile_a[...]

    for r in range(1, SPAN):
        pl.when(~row_later[r])(lambda r=r: rows0[r].start())
    spread(own0[...], wide.at[0])
    def answer_row():
        for r in range(1, SPAN):

            @pl.when(row_later[r])
            def _(r=r):
                pl.semaphore_wait(row_ready.at[r], 1)
                rows0[r].start()

    pl.when(row_shift == 0)(answer_row)

    @pl.when(order < n_col - 1)
    def _():
        pl.semaphore_wait(next_ready, 1)
        up().start()

    pl.when(row_shift == 1)(answer_row)

    def over_pairs(source, count, targets, first, lowest=0):
        def one(pair, carry):
            accumulate(source, count, targets, sums, pair, first)
            return carry

        lax.fori_loop(lowest, SPAN // 2, one, 0)

    def last_block(source, count, targets, give, copies):
        for pair in reversed(range(SPAN // 2)):
            accumulate(source, count, targets, sums, pair, False)
            for k in (2 * pair, 2 * pair + 1):
                for row in range(6):
                    give[k, row : row + 1, :] = jnp.sum(sums[k, row], axis=0, keepdims=True)
                if k > 0:
                    copies[k].start()

    def reduced(give, take, copies, line, lines, act_copies, meet):
        for copy in copies[1:]:
            copy.wait_recv()
        summed = give[0, 0:6, :]
        for r in range(1, SPAN):
            summed = summed + take[r, 0:6, :]
        line[0:6, :] = summed
        for copy in act_copies[1:]:
            copy.start()
        meet()
        for copy in act_copies[1:]:
            copy.wait_recv()
        near = [summed] + [lines[i, 0:6, :] for i in range(1, n_act)]
        while len(near) > 1:
            half = len(near) // 2
            near = [near[i] + near[i + half] for i in range(half)]
        return near[0]

    def corrected(forces, tile):
        acc_old, jerk_old = held[6:9, :], held[9:12, :]
        acc_new, jerk_new = forces[0:3, :], forces[3:6, :]
        pos, vel = correct(acc_old, jerk_old, acc_new, jerk_new, tile[0:3, :], tile[3:6, :])
        held[0:3, :] = pos
        held[3:6, :] = vel
        held[6:9, :] = acc_new
        held[9:12, :] = jerk_new

    def wait_block(b):
        block_copy(own0, b, down_sem.at[b], ordered(order + 1)).wait_recv()

    half = n_col // 2

    def cut(o):
        return jnp.where(o >= n_col - 2, o - half + 1, 0)

    is_last = order == n_col - 1
    passed = jnp.where(is_last, 0, order - cut(order + 1))

    def wraps(t):
        return [
            block_copy(
                own0 if b == 0 else got0.at[b], b, wrap_sem.at[t, b], ordered(n_col - 2 + t)
            )
            for b in range(half - 1 + t)
        ]

    @pl.when(order == 0)
    def _():
        for b in range(1, half):
            wait_block(b)
        for t in range(2):
            pl.semaphore_wait(wrap_ready.at[t], 1)
            for copy in wraps(t):
                copy.start()

    for copy in rows0[1:]:
        copy.wait_recv()
    over_pairs(wide.at[0], part, aim0, True)

    @pl.when(order < n_col - 1)
    def _():
        def forward(j, carry):
            wait_block(order - j)
            pass_up(order - j).start()
            return carry

        lax.fori_loop(1, passed + 1, forward, 0)

    def pull(b):
        spread(got0[b], wide.at[0])
        over_pairs(wide.at[0], part, aim0, False)

    def lower(j, carry):
        pl.when(j > passed)(lambda: wait_block(order - j))
        pull(order - j)
        return carry

    def upper(b, carry):
        pl.when((order > 0) | (b >= half))(lambda: wait_block(b))
        pull(b)
        return carry

    def wrapped(b, carry):
        wait_block(b)
        pull(b)
        return carry

    before_last = order == n_col - 2
    lax.fori_loop(1, jnp.where(is_last, 1, order - cut(order)) + 1, lower, 0)
    lax.fori_loop(order + 1, jnp.where(before_last, n_col, n_col - 1), upper, 0)
    lax.fori_loop(0, jnp.where(before_last, cut(order) - 1, cut(order)), wrapped, 0)
    lax.fori_loop(2, jnp.where(is_last, order - cut(order), 2), lower, 0)
    for i in range(1, n_act):
        pl.when(act_later[i])(lambda i=i: pl.semaphore_wait(act_ready.at[i], 1))
    gives0 = exchange(row_peer, lambda k: give0.at[k, 0:6], take0, row_back, 6)
    acts0 = exchange(act_peer, lambda k: line0.at[0:6], lines0, act_back, 6)
    cols1 = exchange(col_peer, lambda k: own1, got1, col_back)
    final = jnp.where(
        is_last, cut(n_col - 1), jnp.where(before_last, cut(n_col - 2) - 1, n_col - 1)
    )
    wait_block(final)
    spread(got0[final], wide.at[0])
    last_block(wide.at[0], part, aim0, give0, gives0)

    def send_second():
        for q in far_first:
            cols1[n_col - q].start()
        spread(own1[...], wide.at[0])

    corrected(reduced(give0, take0, gives0, line0, lines0, acts0, send_second), tile_a)

    predict_held(tile_b)
    cols2 = exchange(col_peer, lambda k: tile_b, got_act, col_back)
    rows1 = exchange(row_peer, lambda k: tile_b, aim1, row_back)
    cols2[n_col - far_first[0]].start()
    for copy in rows1[1:]:
        copy.start()
    for q in far_first[1:]:
        cols2[n_col - q].start()
    aim1[0] = tile_b[...]
    share = slots // n_act
    first_slot = act * share
    spread_part(tile_b[...], columns, first_slot, share, wide.at[1], 0)
    rows1[1].wait_recv()
    accumulate(wide.at[0], part, aim1, sums, 0, True)
    for n, q in enumerate(near_first[:2]):
        cols1[q].wait_recv()
        spread(got1[q], wide.at[2 + n])
        accumulate(wide.at[2 + n], part, aim1, sums, 0, False)
    for copy in rows1[2:]:
        copy.wait_recv()
    over_pairs(wide.at[0], part, aim1, True, 1)
    over_pairs(wide.at[2], part, aim1, False, 1)
    over_pairs(wide.at[3], part, aim1, False, 1)
    for q in near_first[2:]:
        cols1[q].wait_recv()
        spread(got1[q], wide.at[0])
        over_pairs(wide.at[0], part, aim1, False)
    gives1 = exchange(row_peer, lambda k: give1.at[k, 0:6], take1, row_back, 6)
    acts1 = exchange(act_peer, lambda k: line1.at[0:6], lines1, act_back, 6)
    for n, q in enumerate(near_first[:-1]):
        cols2[q].wait_recv()
        spread_part(got_act[q], columns, first_slot, share, wide.at[1], (n + 1) * share)
    over_pairs(wide.at[1], (n_col - 1) * share, aim1, False)
    cols2[near_first[-1]].wait_recv()
    spread_part(got_act[near_first[-1]], columns, first_slot, share, wide.at[2], 0)
    last_block(wide.at[2], share, aim1, give1, gives1)
    corrected(reduced(give1, take1, gives1, line1, lines1, acts1, lambda: None), tile_b)

    moved = jnp.dot(held[...], hot[...], precision=HIGHEST, preferred_element_type=jnp.float32)
    out_ref[...] = jnp.where(is_active, moved[0:12, :], state_ref[...])
    for copies in (rows0, cols1, gives0, acts0, cols2, rows1, gives1, acts1):
        for copy in copies[1:]:
            copy.wait_send()

    def down_sent(b, carry):
        down(b).wait_send()
        return carry

    lax.fori_loop(0, order, down_sent, 0)

    @pl.when(order < n_col - 1)
    def _():
        up().wait_send()

        def up_sent(b, carry):
            pass_up(b).wait_send()
            return carry

        lax.fori_loop(order - passed, order, up_sent, 0)

    @pl.when(order == 0)
    def _():
        for t in range(2):
            for copy in wraps(t):
                copy.wait_send()


def solution(mesh):
    n_src, n_act = mesh.shape["src"], mesh.shape["act"]
    n_col = n_src // SPAN

    def per_device(star_state, masses, phases, levels, active_list, active_count):
        stars = star_state.shape[1]
        part = stars // n_act
        slots = 2 * active_list.shape[0]
        vmem = pl.BlockSpec(memory_space=pltpu.VMEM)
        n_sem = 2 * n_col + 4 * SPAN + 2 * n_act

        def tiles(*lead):
            return pltpu.VMEM((*lead, 8, 128), jnp.float32)

        return pl.pallas_call(
            functools.partial(kernel, n_src, n_act),
            out_shape=jax.ShapeDtypeStruct(star_state.shape, jnp.float32),
            in_specs=[pl.BlockSpec(memory_space=pl.ANY)] * 4,
            out_specs=vmem,
            scratch_shapes=[
                pltpu.VMEM(star_state.shape, jnp.float32),
                pltpu.VMEM((1, stars), jnp.float32),
                pltpu.VMEM((1, stars), jnp.float32),
                pltpu.VMEM((1, stars), jnp.int32),
                pltpu.SemaphoreType.DMA((4,)),
                pltpu.VMEM((8, part), jnp.float32),
                pltpu.VMEM((8, part), jnp.float32),
                pltpu.VMEM((8, slots), jnp.float32),
                pltpu.VMEM((8, slots), jnp.float32),
                pltpu.VMEM((n_col, 8, part), jnp.float32),
                pltpu.VMEM((n_col, 8, part), jnp.float32),
                pltpu.VMEM((n_col, 8, slots), jnp.float32),
                pltpu.VMEM((SPAN, 8, slots), jnp.float32),
                pltpu.VMEM((SPAN, 8, slots), jnp.float32),
                pltpu.VMEM((4, 7, max(part, n_col * slots // n_act), 128), jnp.float32),
                pltpu.VMEM((slots, 8), jnp.float32),
                tiles(SPAN, 6),
                tiles(SPAN),
                tiles(SPAN),
                tiles(SPAN),
                tiles(SPAN),
                tiles(),
                tiles(),
                tiles(n_act),
                tiles(n_act),
                pltpu.VMEM((slots, stars), jnp.float32),
                pltpu.VMEM((12, slots), jnp.float32),
                pltpu.SemaphoreType.DMA((n_sem,)),
                pltpu.SemaphoreType.DMA((n_sem,)),
                pltpu.SemaphoreType.DMA((n_col,)),
                pltpu.SemaphoreType.DMA((n_col,)),
                pltpu.SemaphoreType.DMA((n_col,)),
                pltpu.SemaphoreType.REGULAR,
                pltpu.SemaphoreType.REGULAR((SPAN,)),
                pltpu.SemaphoreType.REGULAR((n_act,)),
                pltpu.SemaphoreType.DMA((2, n_col)),
                pltpu.SemaphoreType.REGULAR((2,)),
            ],
            compiler_params=pltpu.CompilerParams(collective_id=0, has_side_effects=True),
        )(
            star_state,
            masses.reshape(1, stars),
            phases.reshape(1, stars),
            levels.reshape(1, stars),
        )

    in_specs = (
        P(None, ("groups", "src")),
        P(("groups", "src")),
        P(("groups", "src")),
        P(("groups", "src")),
        P(("groups", "src", "act")),
        P(("groups", "src", "act")),
    )
    return jax.shard_map(
        per_device,
        mesh=mesh,
        in_specs=in_specs,
        out_specs=P(None, ("groups", "src")),
        check_vma=False,
    )
```

```python
import functools

import jax
import jax.numpy as jnp
from jax import lax
from jax.experimental import pallas as pl
from jax.experimental.pallas import tpu as pltpu
from jax.sharding import PartitionSpec as P

LEVELS = 5
STEPS = 2
SPAN = 8

soften_sq = 0.0004
fine_step = 0.03125
MESH = pl.DeviceIdType.MESH
HIGHEST = lax.Precision.HIGHEST


def predict(pos, vel, acc, jerk, interval):
    new_pos = pos + interval * (vel + interval * (0.5 * acc + interval * jerk / 6.0))
    new_vel = vel + interval * (acc + 0.5 * interval * jerk)
    return new_pos, new_vel


def correct(acc_old, jerk_old, acc_new, jerk_new, pos_pred, vel_pred):
    snap_term = (-6.0 * (acc_old - acc_new) - fine_step * (4.0 * jerk_old + 2.0 * jerk_new)) / (
        fine_step * fine_step
    )
    crackle = (12.0 * (acc_old - acc_new) + 6.0 * fine_step * (jerk_old + jerk_new)) / (
        fine_step * fine_step * fine_step
    )
    pos = pos_pred + fine_step**4 / 24.0 * snap_term + fine_step**5 / 120.0 * crackle
    vel = vel_pred + fine_step**3 / 6.0 * snap_term + fine_step**4 / 24.0 * crackle
    return pos, vel


def spread(tile, wide):
    stars = tile.shape[1]
    columns = jnp.transpose(tile)
    for row in range(7):
        wide[row, 0:stars, :] = jnp.broadcast_to(columns[:, row : row + 1], (stars, 128))


def spread_part(tile, columns, begin, count, wide, at):
    columns[...] = jnp.transpose(tile)
    chosen = columns[pl.ds(pl.multiple_of(begin, count), count), :]
    for row in range(7):
        wide[row, at : at + count, :] = jnp.broadcast_to(chosen[:, row : row + 1], (count, 128))


def accumulate(wide, count, targets, sums, pair, first):
    aim = [
        [jnp.broadcast_to(targets[2 * pair + i, row : row + 1, :], (8, 128)) for row in range(6)]
        for i in range(2)
    ]

    def body(step, totals):
        rows = pl.ds(pl.multiple_of(step * 8, 8), 8)
        source = [wide[row, rows, :] for row in range(7)]
        finished = []
        for i in range(2):
            dx, dy, dz, du, dv, dw = [source[row] - aim[i][row] for row in range(6)]
            dist_sq = dx * dx + dy * dy + dz * dz + soften_sq
            inverse = lax.rsqrt(dist_sq)
            inv_sq = inverse * inverse
            weight = source[6] * inverse * inv_sq
            radial = (dx * du + dy * dv + dz * dw) * inv_sq * 3.0
            part = [weight * d for d in (dx, dy, dz)]
            part += [weight * (e - radial * d) for d, e in ((dx, du), (dy, dv), (dz, dw))]
            finished += part
        return tuple(t + p for t, p in zip(totals, finished))

    if first:
        totals = tuple(jnp.zeros((8, 128), jnp.float32) for _ in range(12))
    else:
        totals = tuple(sums[2 * pair + i, row] for i in range(2) for row in range(6))
    totals = lax.fori_loop(0, count // 8, body, totals, unroll=4)
    for i in range(2):
        for row in range(6):
            sums[2 * pair + i, row] = totals[6 * i + row]


def flipped(place, r):
    result, bit = place, 1
    while bit < SPAN:
        if r & bit:
            result = result + bit * (1 - 2 * lax.rem(place // bit, 2))
        bit *= 2
    return result


def kernel(
    n_src,
    n_act,
    state_in,
    mass_in,
    phase_in,
    level_in,
    out_ref,
    state_ref,
    mass_ref,
    phase_ref,
    level_ref,
    in_sem,
    own0,
    own1,
    tile_a,
    tile_b,
    got0,
    got1,
    got_act,
    aim0,
    aim1,
    wide,
    columns,
    sums,
    give0,
    give1,
    take0,
    take1,
    line0,
    line1,
    lines0,
    lines1,
    hot,
    held,
    send_sem,
    recv_sem,
    down_sem,
    up_sem,
    block_sem,
    next_ready,
    row_ready,
    act_ready,
    wrap_sem,
    wrap_ready,
):
    loads = [
        pltpu.make_async_copy(source, target, in_sem.at[k])
        for k, (source, target) in enumerate(
            (
                (state_in, state_ref),
                (mass_in, mass_ref),
                (phase_in, phase_ref),
                (level_in, level_ref),
            )
        )
    ]
    for load in loads:
        load.start()
    n_col = n_src // SPAN
    me = lax.axis_index("src")
    act = lax.axis_index("act")
    group = lax.axis_index("groups")
    place = lax.rem(me, SPAN)
    col = me // SPAN
    base = me - place
    stars = state_ref.shape[1]
    part = stars // n_act
    slots = hot.shape[0]

    col_shift = jnp.where((place == 0) & (act == 0) & (group == 0), 1, 0)
    row_shift = jnp.where((col == 0) & (act == 0) & (group == 0), 1, 0)
    act_shift = jnp.where((me == 0) & (group == 0), 1, 0)
    order = lax.rem(col - col_shift + n_col, n_col)
    row_order = lax.rem(place - row_shift + SPAN, SPAN)
    act_order = lax.rem(act - act_shift + n_act, n_act)

    def ordered(b):
        return {"src": lax.rem(b + col_shift + n_col, n_col) * SPAN + place, "act": act}

    col_peer = [{"src": lax.rem(me + SPAN * q, n_src), "act": act} for q in range(n_col)]
    row_place = [flipped(place, r) for r in range(SPAN)]
    row_peer = [{"src": base + p, "act": act} for p in row_place]
    act_place = [lax.rem(act + i, n_act) for i in range(n_act)]
    act_peer = [{"src": me, "act": a} for a in act_place]
    row_later = [lax.rem(p - row_shift + SPAN, SPAN) > row_order for p in row_place]
    act_later = [lax.rem(a - act_shift + n_act, n_act) > act_order for a in act_place]

    def signal(semaphore, peer):
        pl.semaphore_signal(semaphore, inc=1, device_id=peer, device_id_type=MESH)

    barrier = pltpu.get_barrier_semaphore()

    def greet(b, carry):
        signal(barrier, ordered(b))
        return carry

    lax.fori_loop(order + 1, n_col, greet, 0)
    for later, peers in ((row_later, row_peer), (act_later, act_peer)):
        for k in range(1, len(peers)):
            pl.when(later[k])(functools.partial(signal, barrier, peers[k]))

    counter = [0]

    def exchange(peers, source, target, back, rows=8):
        n = len(peers)
        copies = [None] * n
        for k in range(1, n):
            copies[back(k)] = pltpu.make_async_remote_copy(
                src_ref=source(k),
                dst_ref=target.at[back(k), 0:rows],
                send_sem=send_sem.at[counter[0] + k],
                recv_sem=recv_sem.at[counter[0] + back(k)],
                device_id=peers[k],
                device_id_type=MESH,
            )
        counter[0] += n
        return copies

    def col_back(k):
        return n_col - k

    def row_back(k):
        return k

    def act_back(k):
        return n_act - k

    def block_copy(source, b, semaphore, peer):
        return pltpu.make_async_remote_copy(
            src_ref=source,
            dst_ref=got0.at[b],
            send_sem=semaphore,
            recv_sem=block_sem.at[b],
            device_id=peer,
            device_id_type=MESH,
        )

    def down(b):
        return block_copy(own0, order, down_sem.at[b], ordered(b))

    def up():
        return block_copy(own0, order, up_sem.at[order], ordered(order + 1))

    def pass_up(b):
        return block_copy(got0.at[b], b, up_sem.at[b], ordered(order + 1))

    earlier = order + row_order + act_order
    pl.when(earlier > 0)(lambda: pl.semaphore_wait(barrier, earlier))
    rows0 = exchange(row_peer, lambda k: tile_a, aim0, row_back)
    pl.when(order > 0)(lambda: signal(next_ready, ordered(order - 1)))
    for t in range(2):
        pl.when(order == n_col - 2 + t)(lambda t=t: signal(wrap_ready.at[t], ordered(0)))
    for r in range(1, SPAN):
        pl.when(~row_later[r])(functools.partial(signal, row_ready.at[r], row_peer[r]))
    for i in range(1, n_act):
        pl.when(~act_later[i])(functools.partial(signal, act_ready.at[n_act - i], act_peer[i]))

    for load in loads:
        load.wait()
    total = jnp.float32(stars * n_src)
    mine = pl.ds(pl.multiple_of(act * part, part), part)
    level = level_ref[:, mine]
    tick_count = jnp.left_shift(jnp.int32(1), LEVELS - 1 - level).astype(jnp.float32)
    weight = mass_ref[:, mine] / total

    def predict_own(substep, own):
        elapsed = (
            jnp.where(
                level == LEVELS - 1,
                1.0,
                phase_ref[:, mine] * (tick_count - STEPS) + (substep + 1),
            )
            * fine_step
        )
        pos, vel = predict(
            state_ref[0:3, mine],
            state_ref[3:6, mine],
            state_ref[6:9, mine],
            state_ref[9:12, mine],
            elapsed,
        )
        own[0:3, :] = pos
        own[3:6, :] = vel
        own[6:7, :] = weight if substep == 0 else jnp.where(level == LEVELS - 1, 0.0, weight)
        own[7:8, :] = jnp.zeros((1, part), jnp.float32)

    predict_own(0, own0)
    far_first = sorted(range(1, n_col), key=lambda q: -min(q, n_col - q))
    near_first = far_first[::-1]
    for q in far_first:
        pl.when(order >= q)(lambda q=q: down(order - q).start())

    predict_own(1, own1)
    is_active = level_ref[...] == LEVELS - 1
    flags = jnp.broadcast_to(jnp.where(is_active, 1.0, 0.0), (8, stars))
    before = lax.broadcasted_iota(jnp.int32, (stars, stars), 0) < lax.broadcasted_iota(
        jnp.int32, (stars, stars), 1
    )
    rank = jnp.dot(
        flags.astype(jnp.bfloat16),
        jnp.where(before, 1.0, 0.0).astype(jnp.bfloat16),
        preferred_element_type=jnp.float32,
    )[0:1, :]
    rank = jnp.where(is_active, rank, float(slots)).astype(jnp.int32)
    hot[...] = jnp.where(
        lax.broadcasted_iota(jnp.int32, (slots, stars), 0) == rank, 1.0, 0.0
    )
    over_stars = (((1,), (1,)), ((), ()))
    held[0:12, :] = lax.dot_general(
        state_ref[...], hot[...], over_stars, precision=HIGHEST, preferred_element_type=jnp.float32
    )
    held_mass = lax.dot_general(
        jnp.broadcast_to(mass_ref[...] / total, (8, stars)),
        hot[...],
        over_stars,
        precision=HIGHEST,
        preferred_element_type=jnp.float32,
    )[0:1, :]

    def predict_held(tile):
        pos, vel = predict(
            held[0:3, :], held[3:6, :], held[6:9, :], held[9:12, :], fine_step
        )
        tile[0:3, :] = pos
        tile[3:6, :] = vel
        tile[6:7, :] = held_mass
        tile[7:8, :] = jnp.zeros((1, slots), jnp.float32)

    predict_held(tile_a)
    aim0[0] = tile_a[...]

    for r in range(1, SPAN):
        pl.when(~row_later[r])(lambda r=r: rows0[r].start())
    spread(own0[...], wide.at[0])
    def answer_row():
        for r in range(1, SPAN):

            @pl.when(row_later[r])
            def _(r=r):
                pl.semaphore_wait(row_ready.at[r], 1)
                rows0[r].start()

    pl.when(row_shift == 0)(answer_row)

    @pl.when(order < n_col - 1)
    def _():
        pl.semaphore_wait(next_ready, 1)
        up().start()

    pl.when(row_shift == 1)(answer_row)

    def over_pairs(source, count, targets, first, lowest=0):
        def one(pair, carry):
            accumulate(source, count, targets, sums, pair, first)
            return carry

        lax.fori_loop(lowest, SPAN // 2, one, 0)

    def last_block(source, count, targets, give, copies):
        for pair in reversed(range(SPAN // 2)):
            accumulate(source, count, targets, sums, pair, False)
            for k in (2 * pair, 2 * pair + 1):
                for row in range(6):
                    give[k, row : row + 1, :] = jnp.sum(sums[k, row], axis=0, keepdims=True)
                if k > 0:
                    copies[k].start()

    def reduced(give, take, copies, line, lines, act_copies, meet):
        for copy in copies[1:]:
            copy.wait_recv()
        summed = give[0, 0:6, :]
        for r in range(1, SPAN):
            summed = summed + take[r, 0:6, :]
        line[0:6, :] = summed
        for copy in act_copies[1:]:
            copy.start()
        meet()
        for copy in act_copies[1:]:
            copy.wait_recv()
        near = [summed] + [lines[i, 0:6, :] for i in range(1, n_act)]
        while len(near) > 1:
            half = len(near) // 2
            near = [near[i] + near[i + half] for i in range(half)]
        return near[0]

    def corrected(forces, tile):
        acc_old, jerk_old = held[6:9, :], held[9:12, :]
        acc_new, jerk_new = forces[0:3, :], forces[3:6, :]
        pos, vel = correct(acc_old, jerk_old, acc_new, jerk_new, tile[0:3, :], tile[3:6, :])
        held[0:3, :] = pos
        held[3:6, :] = vel
        held[6:9, :] = acc_new
        held[9:12, :] = jerk_new

    def wait_block(b):
        block_copy(own0, b, down_sem.at[b], ordered(order + 1)).wait_recv()

    half = n_col // 2

    def cut(o):
        return jnp.where(o >= n_col - 2, o - half + 1, 0)

    is_last = order == n_col - 1
    passed = jnp.where(is_last, 0, order - cut(order + 1))

    def wraps(t):
        return [
            block_copy(
                own0 if b == 0 else got0.at[b], b, wrap_sem.at[t, b], ordered(n_col - 2 + t)
            )
            for b in range(half - 1 + t)
        ]

    @pl.when(order == 0)
    def _():
        for b in range(1, half):
            wait_block(b)
        for t in range(2):
            pl.semaphore_wait(wrap_ready.at[t], 1)
            for copy in wraps(t):
                copy.start()

    for copy in rows0[1:]:
        copy.wait_recv()
    over_pairs(wide.at[0], part, aim0, True)

    @pl.when(order < n_col - 1)
    def _():
        def forward(j, carry):
            wait_block(order - j)
            pass_up(order - j).start()
            return carry

        lax.fori_loop(1, passed + 1, forward, 0)

    def pull(b):
        spread(got0[b], wide.at[0])
        over_pairs(wide.at[0], part, aim0, False)

    def lower(j, carry):
        pl.when(j > passed)(lambda: wait_block(order - j))
        pull(order - j)
        return carry

    def upper(b, carry):
        pl.when((order > 0) | (b >= half))(lambda: wait_block(b))
        pull(b)
        return carry

    def wrapped(b, carry):
        wait_block(b)
        pull(b)
        return carry

    before_last = order == n_col - 2
    lax.fori_loop(1, jnp.where(is_last, 1, order - cut(order)) + 1, lower, 0)
    lax.fori_loop(order + 1, jnp.where(before_last, n_col, n_col - 1), upper, 0)
    lax.fori_loop(0, jnp.where(before_last, cut(order) - 1, cut(order)), wrapped, 0)
    lax.fori_loop(2, jnp.where(is_last, order - cut(order), 2), lower, 0)
    for i in range(1, n_act):
        pl.when(act_later[i])(lambda i=i: pl.semaphore_wait(act_ready.at[i], 1))
    gives0 = exchange(row_peer, lambda k: give0.at[k, 0:6], take0, row_back, 6)
    acts0 = exchange(act_peer, lambda k: line0.at[0:6], lines0, act_back, 6)
    cols1 = exchange(col_peer, lambda k: own1, got1, col_back)
    final = jnp.where(
        is_last, cut(n_col - 1), jnp.where(before_last, cut(n_col - 2) - 1, n_col - 1)
    )
    wait_block(final)
    spread(got0[final], wide.at[0])
    last_block(wide.at[0], part, aim0, give0, gives0)

    def send_second():
        for q in far_first:
            cols1[n_col - q].start()
        spread(own1[...], wide.at[0])

    corrected(reduced(give0, take0, gives0, line0, lines0, acts0, send_second), tile_a)

    predict_held(tile_b)
    cols2 = exchange(col_peer, lambda k: tile_b, got_act, col_back)
    rows1 = exchange(row_peer, lambda k: tile_b, aim1, row_back)
    cols2[n_col - far_first[0]].start()
    for copy in rows1[1:]:
        copy.start()
    for q in far_first[1:]:
        cols2[n_col - q].start()
    aim1[0] = tile_b[...]
    share = slots // n_act
    first_slot = act * share
    spread_part(tile_b[...], columns, first_slot, share, wide.at[1], 0)
    rows1[1].wait_recv()
    accumulate(wide.at[0], part, aim1, sums, 0, True)
    for n, q in enumerate(near_first[:2]):
        cols1[q].wait_recv()
        spread(got1[q], wide.at[2 + n])
        accumulate(wide.at[2 + n], part, aim1, sums, 0, False)
    for copy in rows1[2:]:
        copy.wait_recv()
    over_pairs(wide.at[0], part, aim1, True, 1)
    over_pairs(wide.at[2], part, aim1, False, 1)
    over_pairs(wide.at[3], part, aim1, False, 1)
    for q in near_first[2:]:
        cols1[q].wait_recv()
        spread(got1[q], wide.at[0])
        over_pairs(wide.at[0], part, aim1, False)
    gives1 = exchange(row_peer, lambda k: give1.at[k, 0:6], take1, row_back, 6)
    acts1 = exchange(act_peer, lambda k: line1.at[0:6], lines1, act_back, 6)
    for n, q in enumerate(near_first[:-1]):
        cols2[q].wait_recv()
        spread_part(got_act[q], columns, first_slot, share, wide.at[1], (n + 1) * share)
    over_pairs(wide.at[1], (n_col - 1) * share, aim1, False)
    cols2[near_first[-1]].wait_recv()
    spread_part(got_act[near_first[-1]], columns, first_slot, share, wide.at[2], 0)
    last_block(wide.at[2], share, aim1, give1, gives1)
    corrected(reduced(give1, take1, gives1, line1, lines1, acts1, lambda: None), tile_b)

    moved = jnp.dot(held[...], hot[...], precision=HIGHEST, preferred_element_type=jnp.float32)
    out_ref[...] = jnp.where(is_active, moved[0:12, :], state_ref[...])
    for copies in (rows0, cols1, gives0, acts0, cols2, rows1, gives1, acts1):
        for copy in copies[1:]:
            copy.wait_send()

    def down_sent(b, carry):
        down(b).wait_send()
        return carry

    lax.fori_loop(0, order, down_sent, 0)

    @pl.when(order < n_col - 1)
    def _():
        up().wait_send()

        def up_sent(b, carry):
            pass_up(b).wait_send()
            return carry

        lax.fori_loop(order - passed, order, up_sent, 0)

    @pl.when(order == 0)
    def _():
        for t in range(2):
            for copy in wraps(t):
                copy.wait_send()


def solution(mesh):
    n_src, n_act = mesh.shape["src"], mesh.shape["act"]
    n_col = n_src // SPAN

    def per_device(star_state, masses, phases, levels, active_list, active_count):
        stars = star_state.shape[1]
        part = stars // n_act
        slots = 2 * active_list.shape[0]
        vmem = pl.BlockSpec(memory_space=pltpu.VMEM)
        n_sem = 2 * n_col + 4 * SPAN + 2 * n_act

        def tiles(*lead):
            return pltpu.VMEM((*lead, 8, 128), jnp.float32)

        return pl.pallas_call(
            functools.partial(kernel, n_src, n_act),
            out_shape=pltpu.VMEM(star_state.shape, jnp.float32),
            in_specs=[pl.BlockSpec(memory_space=pl.ANY)] * 4,
            out_specs=vmem,
            scratch_shapes=[
                pltpu.VMEM(star_state.shape, jnp.float32),
                pltpu.VMEM((1, stars), jnp.float32),
                pltpu.VMEM((1, stars), jnp.float32),
                pltpu.VMEM((1, stars), jnp.int32),
                pltpu.SemaphoreType.DMA((4,)),
                pltpu.VMEM((8, part), jnp.float32),
                pltpu.VMEM((8, part), jnp.float32),
                pltpu.VMEM((8, slots), jnp.float32),
                pltpu.VMEM((8, slots), jnp.float32),
                pltpu.VMEM((n_col, 8, part), jnp.float32),
                pltpu.VMEM((n_col, 8, part), jnp.float32),
                pltpu.VMEM((n_col, 8, slots), jnp.float32),
                pltpu.VMEM((SPAN, 8, slots), jnp.float32),
                pltpu.VMEM((SPAN, 8, slots), jnp.float32),
                pltpu.VMEM((4, 7, max(part, n_col * slots // n_act), 128), jnp.float32),
                pltpu.VMEM((slots, 8), jnp.float32),
                tiles(SPAN, 6),
                tiles(SPAN),
                tiles(SPAN),
                tiles(SPAN),
                tiles(SPAN),
                tiles(),
                tiles(),
                tiles(n_act),
                tiles(n_act),
                pltpu.VMEM((slots, stars), jnp.float32),
                pltpu.VMEM((12, slots), jnp.float32),
                pltpu.SemaphoreType.DMA((n_sem,)),
                pltpu.SemaphoreType.DMA((n_sem,)),
                pltpu.SemaphoreType.DMA((n_col,)),
                pltpu.SemaphoreType.DMA((n_col,)),
                pltpu.SemaphoreType.DMA((n_col,)),
                pltpu.SemaphoreType.REGULAR,
                pltpu.SemaphoreType.REGULAR((SPAN,)),
                pltpu.SemaphoreType.REGULAR((n_act,)),
                pltpu.SemaphoreType.DMA((2, n_col)),
                pltpu.SemaphoreType.REGULAR((2,)),
            ],
            compiler_params=pltpu.CompilerParams(collective_id=0, has_side_effects=True),
        )(
            star_state,
            masses.reshape(1, stars),
            phases.reshape(1, stars),
            levels.reshape(1, stars),
        )

    in_specs = (
        P(None, ("groups", "src")),
        P(("groups", "src")),
        P(("groups", "src")),
        P(("groups", "src")),
        P(("groups", "src", "act")),
        P(("groups", "src", "act")),
    )
    return jax.shard_map(
        per_device,
        mesh=mesh,
        in_specs=in_specs,
        out_specs=P(None, ("groups", "src")),
        check_vma=False,
    )
```

```python
import functools

import jax
import jax.numpy as jnp
from jax import lax
from jax.experimental import pallas as pl
from jax.experimental.pallas import tpu as pltpu
from jax.sharding import PartitionSpec as P

LEVELS = 5
STEPS = 2
SPAN = 8

soften_sq = 0.0004
fine_step = 0.03125
MESH = pl.DeviceIdType.MESH
HIGHEST = lax.Precision.HIGHEST


def predict(pos, vel, acc, jerk, interval):
    new_pos = pos + interval * (vel + interval * (0.5 * acc + interval * jerk / 6.0))
    new_vel = vel + interval * (acc + 0.5 * interval * jerk)
    return new_pos, new_vel


def correct(acc_old, jerk_old, acc_new, jerk_new, pos_pred, vel_pred):
    snap_term = (-6.0 * (acc_old - acc_new) - fine_step * (4.0 * jerk_old + 2.0 * jerk_new)) / (
        fine_step * fine_step
    )
    crackle = (12.0 * (acc_old - acc_new) + 6.0 * fine_step * (jerk_old + jerk_new)) / (
        fine_step * fine_step * fine_step
    )
    pos = pos_pred + fine_step**4 / 24.0 * snap_term + fine_step**5 / 120.0 * crackle
    vel = vel_pred + fine_step**3 / 6.0 * snap_term + fine_step**4 / 24.0 * crackle
    return pos, vel


def spread(tile, wide):
    stars = tile.shape[1]
    columns = jnp.transpose(tile)
    for row in range(7):
        wide[row, 0:stars, :] = jnp.broadcast_to(columns[:, row : row + 1], (stars, 128))


def spread_part(tile, columns, begin, count, wide, at):
    columns[...] = jnp.transpose(tile)
    chosen = columns[pl.ds(pl.multiple_of(begin, count), count), :]
    for row in range(7):
        wide[row, at : at + count, :] = jnp.broadcast_to(chosen[:, row : row + 1], (count, 128))


def accumulate(wide, count, targets, sums, pair, first):
    aim = [
        [jnp.broadcast_to(targets[2 * pair + i, row : row + 1, :], (8, 128)) for row in range(6)]
        for i in range(2)
    ]

    def body(step, totals):
        rows = pl.ds(pl.multiple_of(step * 8, 8), 8)
        source = [wide[row, rows, :] for row in range(7)]
        finished = []
        for i in range(2):
            dx, dy, dz, du, dv, dw = [source[row] - aim[i][row] for row in range(6)]
            dist_sq = dx * dx + dy * dy + dz * dz + soften_sq
            inverse = lax.rsqrt(dist_sq)
            inv_sq = inverse * inverse
            weight = source[6] * inverse * inv_sq
            radial = (dx * du + dy * dv + dz * dw) * inv_sq * 3.0
            part = [weight * d for d in (dx, dy, dz)]
            part += [weight * (e - radial * d) for d, e in ((dx, du), (dy, dv), (dz, dw))]
            finished += part
        return tuple(t + p for t, p in zip(totals, finished))

    if first:
        totals = tuple(jnp.zeros((8, 128), jnp.float32) for _ in range(12))
    else:
        totals = tuple(sums[2 * pair + i, row] for i in range(2) for row in range(6))
    steps = count // 8
    totals = lax.fori_loop(0, steps, body, totals, unroll=4 if steps % 8 else 8)
    for i in range(2):
        for row in range(6):
            sums[2 * pair + i, row] = totals[6 * i + row]


def flipped(place, r):
    result, bit = place, 1
    while bit < SPAN:
        if r & bit:
            result = result + bit * (1 - 2 * lax.rem(place // bit, 2))
        bit *= 2
    return result


def kernel(
    n_src,
    n_act,
    state_in,
    mass_in,
    phase_in,
    level_in,
    out_ref,
    state_ref,
    mass_ref,
    phase_ref,
    level_ref,
    in_sem,
    own0,
    own1,
    tile_a,
    tile_b,
    got0,
    got1,
    got_act,
    aim0,
    aim1,
    wide,
    columns,
    sums,
    give0,
    give1,
    take0,
    take1,
    line0,
    line1,
    lines0,
    lines1,
    hot,
    held,
    send_sem,
    recv_sem,
    down_sem,
    up_sem,
    block_sem,
    next_ready,
    row_ready,
    act_ready,
    wrap_sem,
    wrap_ready,
):
    loads = [
        pltpu.make_async_copy(source, target, in_sem.at[k])
        for k, (source, target) in enumerate(
            (
                (state_in, state_ref),
                (mass_in, mass_ref),
                (phase_in, phase_ref),
                (level_in, level_ref),
            )
        )
    ]
    for load in loads:
        load.start()
    n_col = n_src // SPAN
    me = lax.axis_index("src")
    act = lax.axis_index("act")
    group = lax.axis_index("groups")
    place = lax.rem(me, SPAN)
    col = me // SPAN
    base = me - place
    stars = state_ref.shape[1]
    part = stars // n_act
    slots = hot.shape[0]

    col_shift = jnp.where((place == 0) & (act == 0) & (group == 0), 1, 0)
    row_shift = jnp.where((col == 0) & (act == 0) & (group == 0), 1, 0)
    act_shift = jnp.where((me == 0) & (group == 0), 1, 0)
    order = lax.rem(col - col_shift + n_col, n_col)
    row_order = lax.rem(place - row_shift + SPAN, SPAN)
    act_order = lax.rem(act - act_shift + n_act, n_act)

    def ordered(b):
        return {"src": lax.rem(b + col_shift + n_col, n_col) * SPAN + place, "act": act}

    col_peer = [{"src": lax.rem(me + SPAN * q, n_src), "act": act} for q in range(n_col)]
    row_place = [flipped(place, r) for r in range(SPAN)]
    row_peer = [{"src": base + p, "act": act} for p in row_place]
    act_place = [lax.rem(act + i, n_act) for i in range(n_act)]
    act_peer = [{"src": me, "act": a} for a in act_place]
    row_later = [lax.rem(p - row_shift + SPAN, SPAN) > row_order for p in row_place]
    act_later = [lax.rem(a - act_shift + n_act, n_act) > act_order for a in act_place]

    def signal(semaphore, peer):
        pl.semaphore_signal(semaphore, inc=1, device_id=peer, device_id_type=MESH)

    barrier = pltpu.get_barrier_semaphore()

    def greet(b, carry):
        signal(barrier, ordered(b))
        return carry

    lax.fori_loop(order + 1, n_col, greet, 0)
    for later, peers in ((row_later, row_peer), (act_later, act_peer)):
        for k in range(1, len(peers)):
            pl.when(later[k])(functools.partial(signal, barrier, peers[k]))

    counter = [0]

    def exchange(peers, source, target, back, rows=8):
        n = len(peers)
        copies = [None] * n
        for k in range(1, n):
            copies[back(k)] = pltpu.make_async_remote_copy(
                src_ref=source(k),
                dst_ref=target.at[back(k), 0:rows],
                send_sem=send_sem.at[counter[0] + k],
                recv_sem=recv_sem.at[counter[0] + back(k)],
                device_id=peers[k],
                device_id_type=MESH,
            )
        counter[0] += n
        return copies

    def col_back(k):
        return n_col - k

    def row_back(k):
        return k

    def act_back(k):
        return n_act - k

    def block_copy(source, b, semaphore, peer):
        return pltpu.make_async_remote_copy(
            src_ref=source,
            dst_ref=got0.at[b],
            send_sem=semaphore,
            recv_sem=block_sem.at[b],
            device_id=peer,
            device_id_type=MESH,
        )

    def down(b):
        return block_copy(own0, order, down_sem.at[b], ordered(b))

    def up():
        return block_copy(own0, order, up_sem.at[order], ordered(order + 1))

    def pass_up(b):
        return block_copy(got0.at[b], b, up_sem.at[b], ordered(order + 1))

    earlier = order + row_order + act_order
    pl.when(earlier > 0)(lambda: pl.semaphore_wait(barrier, earlier))
    rows0 = exchange(row_peer, lambda k: tile_a, aim0, row_back)
    pl.when(order > 0)(lambda: signal(next_ready, ordered(order - 1)))
    for t in range(2):
        pl.when(order == n_col - 2 + t)(lambda t=t: signal(wrap_ready.at[t], ordered(0)))
    for r in range(1, SPAN):
        pl.when(~row_later[r])(functools.partial(signal, row_ready.at[r], row_peer[r]))
    for i in range(1, n_act):
        pl.when(~act_later[i])(functools.partial(signal, act_ready.at[n_act - i], act_peer[i]))

    for load in loads:
        load.wait()
    total = jnp.float32(stars * n_src)
    mine = pl.ds(pl.multiple_of(act * part, part), part)
    level = level_ref[:, mine]
    tick_count = jnp.left_shift(jnp.int32(1), LEVELS - 1 - level).astype(jnp.float32)
    weight = mass_ref[:, mine] / total

    def predict_own(substep, own):
        elapsed = (
            jnp.where(
                level == LEVELS - 1,
                1.0,
                phase_ref[:, mine] * (tick_count - STEPS) + (substep + 1),
            )
            * fine_step
        )
        pos, vel = predict(
            state_ref[0:3, mine],
            state_ref[3:6, mine],
            state_ref[6:9, mine],
            state_ref[9:12, mine],
            elapsed,
        )
        own[0:3, :] = pos
        own[3:6, :] = vel
        own[6:7, :] = weight if substep == 0 else jnp.where(level == LEVELS - 1, 0.0, weight)
        own[7:8, :] = jnp.zeros((1, part), jnp.float32)

    predict_own(0, own0)
    far_first = sorted(range(1, n_col), key=lambda q: -min(q, n_col - q))
    near_first = far_first[::-1]
    for q in far_first:
        pl.when(order >= q)(lambda q=q: down(order - q).start())

    predict_own(1, own1)
    is_active = level_ref[...] == LEVELS - 1
    flags = jnp.broadcast_to(jnp.where(is_active, 1.0, 0.0), (8, stars))
    before = lax.broadcasted_iota(jnp.int32, (stars, stars), 0) < lax.broadcasted_iota(
        jnp.int32, (stars, stars), 1
    )
    rank = jnp.dot(
        flags.astype(jnp.bfloat16),
        jnp.where(before, 1.0, 0.0).astype(jnp.bfloat16),
        preferred_element_type=jnp.float32,
    )[0:1, :]
    rank = jnp.where(is_active, rank, float(slots)).astype(jnp.int32)
    hot[...] = jnp.where(
        lax.broadcasted_iota(jnp.int32, (slots, stars), 0) == rank, 1.0, 0.0
    )
    over_stars = (((1,), (1,)), ((), ()))
    held[0:12, :] = lax.dot_general(
        state_ref[...], hot[...], over_stars, precision=HIGHEST, preferred_element_type=jnp.float32
    )
    held_mass = lax.dot_general(
        jnp.broadcast_to(mass_ref[...] / total, (8, stars)),
        hot[...],
        over_stars,
        precision=HIGHEST,
        preferred_element_type=jnp.float32,
    )[0:1, :]

    def predict_held(tile):
        pos, vel = predict(
            held[0:3, :], held[3:6, :], held[6:9, :], held[9:12, :], fine_step
        )
        tile[0:3, :] = pos
        tile[3:6, :] = vel
        tile[6:7, :] = held_mass
        tile[7:8, :] = jnp.zeros((1, slots), jnp.float32)

    predict_held(tile_a)
    aim0[0] = tile_a[...]

    for r in range(1, SPAN):
        pl.when(~row_later[r])(lambda r=r: rows0[r].start())
    spread(own0[...], wide.at[0])
    def answer_row():
        for r in range(1, SPAN):

            @pl.when(row_later[r])
            def _(r=r):
                pl.semaphore_wait(row_ready.at[r], 1)
                rows0[r].start()

    pl.when(row_shift == 0)(answer_row)

    @pl.when(order < n_col - 1)
    def _():
        pl.semaphore_wait(next_ready, 1)
        up().start()

    pl.when(row_shift == 1)(answer_row)

    def over_pairs(source, count, targets, first, lowest=0):
        def one(pair, carry):
            accumulate(source, count, targets, sums, pair, first)
            return carry

        lax.fori_loop(lowest, SPAN // 2, one, 0)

    def last_block(source, count, targets, give, copies):
        for pair in reversed(range(SPAN // 2)):
            accumulate(source, count, targets, sums, pair, False)
            for k in (2 * pair, 2 * pair + 1):
                for row in range(6):
                    give[k, row : row + 1, :] = jnp.sum(sums[k, row], axis=0, keepdims=True)
                if k > 0:
                    copies[k].start()

    def reduced(give, take, copies, line, lines, act_copies, meet):
        for copy in copies[1:]:
            copy.wait_recv()
        summed = give[0, 0:6, :]
        for r in range(1, SPAN):
            summed = summed + take[r, 0:6, :]
        line[0:6, :] = summed
        for copy in act_copies[1:]:
            copy.start()
        meet()
        for copy in act_copies[1:]:
            copy.wait_recv()
        near = [summed] + [lines[i, 0:6, :] for i in range(1, n_act)]
        while len(near) > 1:
            half = len(near) // 2
            near = [near[i] + near[i + half] for i in range(half)]
        return near[0]

    def corrected(forces, tile):
        acc_old, jerk_old = held[6:9, :], held[9:12, :]
        acc_new, jerk_new = forces[0:3, :], forces[3:6, :]
        pos, vel = correct(acc_old, jerk_old, acc_new, jerk_new, tile[0:3, :], tile[3:6, :])
        held[0:3, :] = pos
        held[3:6, :] = vel
        held[6:9, :] = acc_new
        held[9:12, :] = jerk_new

    def wait_block(b):
        block_copy(own0, b, down_sem.at[b], ordered(order + 1)).wait_recv()

    half = n_col // 2

    def cut(o):
        return jnp.where(o >= n_col - 2, o - half + 1, 0)

    is_last = order == n_col - 1
    passed = jnp.where(is_last, 0, order - cut(order + 1))

    def wraps(t):
        return [
            block_copy(
                own0 if b == 0 else got0.at[b], b, wrap_sem.at[t, b], ordered(n_col - 2 + t)
            )
            for b in range(half - 1 + t)
        ]

    @pl.when(order == 0)
    def _():
        for b in range(1, half):
            wait_block(b)
        for t in range(2):
            pl.semaphore_wait(wrap_ready.at[t], 1)
            for copy in wraps(t):
                copy.start()

    for copy in rows0[1:]:
        copy.wait_recv()
    over_pairs(wide.at[0], part, aim0, True)

    @pl.when(order < n_col - 1)
    def _():
        def forward(j, carry):
            wait_block(order - j)
            pass_up(order - j).start()
            return carry

        lax.fori_loop(1, passed + 1, forward, 0)

    def pull(b):
        spread(got0[b], wide.at[0])
        over_pairs(wide.at[0], part, aim0, False)

    def lower(j, carry):
        pl.when(j > passed)(lambda: wait_block(order - j))
        pull(order - j)
        return carry

    def upper(b, carry):
        pl.when((order > 0) | (b >= half))(lambda: wait_block(b))
        pull(b)
        return carry

    def wrapped(b, carry):
        wait_block(b)
        pull(b)
        return carry

    before_last = order == n_col - 2
    lax.fori_loop(1, jnp.where(is_last, 1, order - cut(order)) + 1, lower, 0)
    lax.fori_loop(order + 1, jnp.where(before_last, n_col, n_col - 1), upper, 0)
    lax.fori_loop(0, jnp.where(before_last, cut(order) - 1, cut(order)), wrapped, 0)
    lax.fori_loop(2, jnp.where(is_last, order - cut(order), 2), lower, 0)
    for i in range(1, n_act):
        pl.when(act_later[i])(lambda i=i: pl.semaphore_wait(act_ready.at[i], 1))
    gives0 = exchange(row_peer, lambda k: give0.at[k, 0:6], take0, row_back, 6)
    acts0 = exchange(act_peer, lambda k: line0.at[0:6], lines0, act_back, 6)
    cols1 = exchange(col_peer, lambda k: own1, got1, col_back)
    final = jnp.where(
        is_last, cut(n_col - 1), jnp.where(before_last, cut(n_col - 2) - 1, n_col - 1)
    )
    wait_block(final)
    spread(got0[final], wide.at[0])
    last_block(wide.at[0], part, aim0, give0, gives0)

    def send_second():
        for q in far_first:
            cols1[n_col - q].start()
        spread(own1[...], wide.at[0])

    corrected(reduced(give0, take0, gives0, line0, lines0, acts0, send_second), tile_a)

    predict_held(tile_b)
    cols2 = exchange(col_peer, lambda k: tile_b, got_act, col_back)
    rows1 = exchange(row_peer, lambda k: tile_b, aim1, row_back)
    cols2[n_col - far_first[0]].start()
    for copy in rows1[1:]:
        copy.start()
    for q in far_first[1:]:
        cols2[n_col - q].start()
    aim1[0] = tile_b[...]
    share = slots // n_act
    first_slot = act * share
    spread_part(tile_b[...], columns, first_slot, share, wide.at[1], 0)
    rows1[1].wait_recv()
    accumulate(wide.at[0], part, aim1, sums, 0, True)
    for n, q in enumerate(near_first[:2]):
        cols1[q].wait_recv()
        spread(got1[q], wide.at[2 + n])
        accumulate(wide.at[2 + n], part, aim1, sums, 0, False)
    for copy in rows1[2:]:
        copy.wait_recv()
    over_pairs(wide.at[0], part, aim1, True, 1)
    over_pairs(wide.at[2], part, aim1, False, 1)
    over_pairs(wide.at[3], part, aim1, False, 1)
    for q in near_first[2:]:
        cols1[q].wait_recv()
        spread(got1[q], wide.at[0])
        over_pairs(wide.at[0], part, aim1, False)
    gives1 = exchange(row_peer, lambda k: give1.at[k, 0:6], take1, row_back, 6)
    acts1 = exchange(act_peer, lambda k: line1.at[0:6], lines1, act_back, 6)
    for n, q in enumerate(near_first[:-1]):
        cols2[q].wait_recv()
        spread_part(got_act[q], columns, first_slot, share, wide.at[1], (n + 1) * share)
    over_pairs(wide.at[1], (n_col - 1) * share, aim1, False)
    cols2[near_first[-1]].wait_recv()
    spread_part(got_act[near_first[-1]], columns, first_slot, share, wide.at[2], 0)
    last_block(wide.at[2], share, aim1, give1, gives1)
    corrected(reduced(give1, take1, gives1, line1, lines1, acts1, lambda: None), tile_b)

    moved = jnp.dot(held[...], hot[...], precision=HIGHEST, preferred_element_type=jnp.float32)
    out_ref[...] = jnp.where(is_active, moved[0:12, :], state_ref[...])
    for copies in (rows0, cols1, gives0, acts0, cols2, rows1, gives1, acts1):
        for copy in copies[1:]:
            copy.wait_send()

    def down_sent(b, carry):
        down(b).wait_send()
        return carry

    lax.fori_loop(0, order, down_sent, 0)

    @pl.when(order < n_col - 1)
    def _():
        up().wait_send()

        def up_sent(b, carry):
            pass_up(b).wait_send()
            return carry

        lax.fori_loop(order - passed, order, up_sent, 0)

    @pl.when(order == 0)
    def _():
        for t in range(2):
            for copy in wraps(t):
                copy.wait_send()


def solution(mesh):
    n_src, n_act = mesh.shape["src"], mesh.shape["act"]
    n_col = n_src // SPAN

    def per_device(star_state, masses, phases, levels, active_list, active_count):
        stars = star_state.shape[1]
        part = stars // n_act
        slots = 2 * active_list.shape[0]
        vmem = pl.BlockSpec(memory_space=pltpu.VMEM)
        n_sem = 2 * n_col + 4 * SPAN + 2 * n_act

        def tiles(*lead):
            return pltpu.VMEM((*lead, 8, 128), jnp.float32)

        return pl.pallas_call(
            functools.partial(kernel, n_src, n_act),
            out_shape=pltpu.VMEM(star_state.shape, jnp.float32),
            in_specs=[pl.BlockSpec(memory_space=pl.ANY)] * 4,
            out_specs=vmem,
            scratch_shapes=[
                pltpu.VMEM(star_state.shape, jnp.float32),
                pltpu.VMEM((1, stars), jnp.float32),
                pltpu.VMEM((1, stars), jnp.float32),
                pltpu.VMEM((1, stars), jnp.int32),
                pltpu.SemaphoreType.DMA((4,)),
                pltpu.VMEM((8, part), jnp.float32),
                pltpu.VMEM((8, part), jnp.float32),
                pltpu.VMEM((8, slots), jnp.float32),
                pltpu.VMEM((8, slots), jnp.float32),
                pltpu.VMEM((n_col, 8, part), jnp.float32),
                pltpu.VMEM((n_col, 8, part), jnp.float32),
                pltpu.VMEM((n_col, 8, slots), jnp.float32),
                pltpu.VMEM((SPAN, 8, slots), jnp.float32),
                pltpu.VMEM((SPAN, 8, slots), jnp.float32),
                pltpu.VMEM((4, 7, max(part, n_col * slots // n_act), 128), jnp.float32),
                pltpu.VMEM((slots, 8), jnp.float32),
                tiles(SPAN, 6),
                tiles(SPAN),
                tiles(SPAN),
                tiles(SPAN),
                tiles(SPAN),
                tiles(),
                tiles(),
                tiles(n_act),
                tiles(n_act),
                pltpu.VMEM((slots, stars), jnp.float32),
                pltpu.VMEM((12, slots), jnp.float32),
                pltpu.SemaphoreType.DMA((n_sem,)),
                pltpu.SemaphoreType.DMA((n_sem,)),
                pltpu.SemaphoreType.DMA((n_col,)),
                pltpu.SemaphoreType.DMA((n_col,)),
                pltpu.SemaphoreType.DMA((n_col,)),
                pltpu.SemaphoreType.REGULAR,
                pltpu.SemaphoreType.REGULAR((SPAN,)),
                pltpu.SemaphoreType.REGULAR((n_act,)),
                pltpu.SemaphoreType.DMA((2, n_col)),
                pltpu.SemaphoreType.REGULAR((2,)),
            ],
            compiler_params=pltpu.CompilerParams(collective_id=0, has_side_effects=True),
        )(
            star_state,
            masses.reshape(1, stars),
            phases.reshape(1, stars),
            levels.reshape(1, stars),
        )

    in_specs = (
        P(None, ("groups", "src")),
        P(("groups", "src")),
        P(("groups", "src")),
        P(("groups", "src")),
        P(("groups", "src", "act")),
        P(("groups", "src", "act")),
    )
    return jax.shard_map(
        per_device,
        mesh=mesh,
        in_specs=in_specs,
        out_specs=P(None, ("groups", "src")),
        check_vma=False,
    )
```
